128 devices in a mesh: sx: 16 (over x, y_lo, core), sy: 8 (over z, y_hi).
Axes of the slice: x: 4, y: 4 (y_hi: 2, y_lo: 2; y = y_hi * 2 + y_lo), z: 4, core: 2. Of those that a mesh axis runs over, the one named last changes fastest.
Arguments:
- queries: bfloat16 [8192, 128, 128], P(('sx', 'sy')), may hold values from -8 to 8
- keys: bfloat16 [8192, 8, 128], P(('sx', 'sy')), may hold values from -8 to 8
- values: bfloat16 [8192, 8, 128], P(('sx', 'sy')), may hold values from -6 to 6
Outputs:
- attention: bfloat16 [8192, 128, 128], P(('sx', 'sy'))
The draws below stay inside these ranges and needn't reach their ends.
All inputs are finite; a program needn't handle non-finite values.
Results may differ from the reference program's by a relative error of at most 0.005.
Values may be sent and summed in bfloat16 or wider, within the bound.
A program may use at most 64 MiB of HBM per device.

```python
import math
import jax
import jax.numpy as jnp
from jax import lax

HEAD_DIM = 128
HEADS = 128
KV_HEADS = 8
TOKENS = 8192


def shard_levels(own_key, dims, shards, low, high):
    loudness = 1.0
    for axis_at, shards_of in shards:
        heights = jax.random.uniform(jax.random.fold_in(jax.random.fold_in(own_key, 6), axis_at), (shards_of,), jnp.float32, low / len(shards), high / len(shards))
        loudness = loudness * jnp.repeat(jnp.exp(heights), dims[axis_at] // shards_of).reshape((-1,) + (1,) * (len(dims) - 1 - axis_at))
    return loudness


def noise(key, shape, width, most, cuts=(), kind=jnp.bfloat16):
    entries = jax.random.normal(key, shape, jnp.float32) * width
    if len(cuts) > 0:
        entries = shard_levels(key, shape, cuts, -0.22, 0.18) * entries
    return jnp.clip(entries, min=-most, max=most).astype(kind)


def setup_inputs(seed: int = 0) -> dict:
    key_of = jax.random.split(jax.random.key(seed), 4)
    return {
        "queries": noise(key_of[0], (TOKENS, HEADS, HEAD_DIM), 1.6, 8.0, ((0, 128),)),
        "keys": noise(key_of[1], (TOKENS, KV_HEADS, HEAD_DIM), 1.6, 8.0, ((0, 128),)),
        "values": noise(key_of[2], (TOKENS, KV_HEADS, HEAD_DIM), 1.0, 6.0, ((0, 128),)),
    }


def frequencies(head_width):
    half_index = jnp.arange(head_width // 2, dtype=jnp.float32)
    base_rate = jnp.power(jnp.float32(500000.0), -2.0 * half_index / head_width)
    wavelen = 2.0 * math.pi / base_rate
    smooth = (8192.0 / wavelen - 1.0) / 3.0
    blended = (1.0 - smooth) * base_rate / 8.0 + smooth * base_rate
    return jnp.where(wavelen < 2048.0, base_rate, jnp.where(wavelen > 8192.0, base_rate / 8.0, blended))

def rotate(heads_in, positions):
    head_width = heads_in.shape[-1]
    half_width = head_width // 2
    angles = positions.astype(jnp.float32)[:, None] * frequencies(head_width)[None, :]
    cosine = jnp.cos(angles)[:, None, :]
    sine_wave = jnp.sin(angles)[:, None, :]
    widened = heads_in.astype(jnp.float32)
    front = widened[..., :half_width]
    second = widened[..., half_width:]
    turned = jnp.concatenate([front * cosine - second * sine_wave, second * cosine + front * sine_wave], axis=-1)
    return turned.astype(jnp.bfloat16)

def reference(queries, keys, values):
    total_rows, heads_all, head_width = queries.shape
    group_size = heads_all // keys.shape[1]
    positions = jnp.arange(total_rows, dtype=jnp.int32)
    query_rot = lax.optimization_barrier(rotate(queries, positions))
    key_rot = lax.optimization_barrier(rotate(keys, positions))
    score_scale = 1.0 / math.sqrt(head_width)
    block_size = total_rows // 8

    def one_head(head_index):
        query_head = lax.dynamic_index_in_dim(query_rot, head_index, 1, keepdims=False)
        key_index = (head_index // group_size).astype(jnp.int32)
        key_head = lax.dynamic_index_in_dim(key_rot, key_index, 1, keepdims=False)
        value_head = lax.dynamic_index_in_dim(values, key_index, 1, keepdims=False)
        pieces = []
        for block_index in range(8):
            row_begin = block_index * block_size
            key_end = row_begin + block_size
            query_rows = query_head[row_begin:key_end]
            scores = jnp.dot(query_rows, key_head[:key_end].T, preferred_element_type=jnp.float32) * score_scale
            allowed = positions[:key_end][None, :] <= positions[row_begin:key_end][:, None]
            scores = jnp.where(allowed, scores, -jnp.inf)
            weights = jnp.exp(scores - lax.optimization_barrier(jnp.max(scores, axis=1, keepdims=True)))
            summed = jnp.dot(weights.astype(jnp.bfloat16), value_head[:key_end], preferred_element_type=jnp.float32)
            pieces.append(summed / lax.optimization_barrier(jnp.sum(weights, axis=1, keepdims=True)))
        return jnp.concatenate(pieces, axis=0).astype(jnp.bfloat16)
    result = lax.map(one_head, jnp.arange(heads_all, dtype=jnp.int32))
    return jnp.transpose(result, (1, 0, 2))
```

```python
import functools
import math

import jax
import jax.numpy as jnp
from jax import lax
from jax.experimental import pallas as pl
from jax.experimental.pallas import tpu as pltpu
from jax.sharding import PartitionSpec as P

MESH = pl.DeviceIdType.MESH
F32 = jnp.float32
BF16 = jnp.bfloat16
NEG = -1e30
CW = 256
QW = 1024
KB = 512
VR = 144
UNITS = 68
SCALE = math.log2(math.e) / math.sqrt(128.0)


def frequencies(head_width):
    half_index = jnp.arange(head_width // 2, dtype=F32)
    base_rate = jnp.power(F32(500000.0), -2.0 * half_index / head_width)
    wavelen = 2.0 * math.pi / base_rate
    smooth = (8192.0 / wavelen - 1.0) / 3.0
    blended = (1.0 - smooth) * base_rate / 8.0 + smooth * base_rate
    return jnp.where(
        wavelen < 2048.0, base_rate, jnp.where(wavelen > 8192.0, base_rate / 8.0, blended)
    )


def place(p, b):
    return jnp.where(b == 0, p, 3 - p)


class Spot:
    def __init__(self, p, b, core):
        self.p, self.b, self.core = tuple(p), tuple(b), core

    @staticmethod
    def own():
        sx, sy = lax.axis_index("sx"), lax.axis_index("sy")
        xyz = (sx // 4, (sy % 2) * 2 + (sx // 2) % 2, sy // 2)
        return Spot([((c + 1) // 2) % 2 for c in xyz], [c // 2 for c in xyz], sx % 2)

    @property
    def sx(self):
        ylo = (self.p[1] + self.b[1]) % 2
        return place(self.p[0], self.b[0]) * 4 + ylo * 2 + self.core

    @property
    def sy(self):
        return place(self.p[2], self.b[2]) * 2 + self.b[1]

    @property
    def device(self):
        return (self.sx, self.sy)

    @property
    def chip(self):
        return self.b[0] * 4 + self.b[1] * 2 + self.b[2]

    @property
    def head_block(self):
        return self.chip * 2 + self.core

    @property
    def pair_block(self):
        return (self.b[0] * 2 + self.b[1]) * 2 + self.core

    @property
    def slot(self):
        return self.pair_block * 2 + self.b[2]

    @property
    def part(self):
        return self.p[1] * 2 + self.p[2]

    def member(self, d, dc):
        return Spot(self.p, [(b + (d >> s) % 2) % 2 for b, s in zip(self.b, (2, 1, 0))], (self.core + dc) % 2)

    def cousin(self, d):
        return Spot([(p + (d >> s) % 2) % 2 for p, s in zip(self.p, (2, 1, 0))], self.b, self.core)


ORDER = (7, 3, 5, 6, 1, 2, 4, 0)


def kernel(q_ref, kv_ref, cos_ref, sin_ref, out_ref,
           qs, qr, kvb, ost, qT, vT, s0, s1, s2, s3, p0, p1, p2, p3, mx, al, m_ref, acc_ref,
           q_send, q_recv, k1_send, k1_recv, k2_send, k2_recv, f_send, f_recv, o_send, o_recv):
    S, W = (s0, s1, s2, s3), (p0, p1, p2, p3)
    H = CW // 128
    me = Spot.own()
    others = [(d, dc) for d in ORDER for dc in (1, 0) if (d, dc) != (0, 0)]

    def remote(src, dst, send, recv, spot):
        return pltpu.make_async_remote_copy(src_ref=src, dst_ref=dst, send_sem=send, recv_sem=recv, device_id=spot.device, device_id_type=MESH)

    barrier = pltpu.get_barrier_semaphore()
    for d, dc in others:
        pl.semaphore_signal(barrier, inc=1, device_id=me.member(d, dc).device, device_id_type=MESH)
    for d in range(1, 8):
        pl.semaphore_signal(barrier, inc=1, device_id=me.cousin(d).device, device_id_type=MESH)
    pl.semaphore_wait(barrier, len(others) + 7)

    def kv_spot(role, src):
        return kvb.at[role, src.sx, src.part, pl.ds(pl.multiple_of(src.b[2] * 64, 64), 64), :]

    def first(d, dc):
        to = me.member(d, dc)
        return remote(kv_ref.at[to.core, to.chip], kv_spot(to.core, me), k1_send.at[d * 2 + dc], k1_recv.at[me.slot], to)

    for d, dc in others:
        first(d, dc).start()
    kvb[me.core, me.sx, me.part, pl.ds(pl.multiple_of(me.b[2] * 64, 64), 64), :] = kv_ref[me.core, me.chip]

    def queries_to(d, dc):
        to = me.member(d, dc)
        return remote(qs.at[to.head_block], qr.at[me.slot], q_send.at[d * 2 + dc], q_recv.at[me.slot], to)

    for d in ORDER:
        to = me.member(d, 0)
        x = q_ref[:, pl.ds(pl.multiple_of(to.chip * 16, 16), 16), :].astype(F32)
        for c in range(2):
            part = x[:, c * 8:(c + 1) * 8, :].reshape(512, 128)
            turned = part * cos_ref[...] + pltpu.roll(part, 64, 1) * sin_ref[...]
            qs[to.chip * 2 + c] = turned.astype(BF16)
        for dc in (1, 0):
            if (d, dc) != (0, 0):
                queries_to(d, dc).start()
    qr[me.slot] = qs[me.head_block]

    for d, dc in others:
        frm = me.member(d, dc)
        remote(kv_ref.at[0, 0], kv_spot(me.core, frm), k1_send.at[d * 2 + dc], k1_recv.at[frm.slot], frm).wait_recv()

    def region(spot, half):
        return kvb.at[me.core, pl.ds(pl.multiple_of(place(spot.p[0], half) * 4, 4), 4), spot.part]

    def second(d, half):
        r = region(me, half)
        return remote(r, r, k2_send.at[d * 2 + half], k2_recv.at[d * 2 + half], me.cousin(d))

    def forward(d, half):
        r = region(me.cousin(d), half)
        return remote(r, r, f_send.at[d * 2 + half], f_recv.at[d * 2 + half], me.member(0, 1))

    for d in (7, 3, 5, 6, 1, 2, 4):
        for half in range(2):
            second(d, half).start()
    for half in range(2):
        forward(0, half).start()
    for d in (4, 2, 1, 6, 5, 3, 7):
        for half in range(2):
            r = region(me.cousin(d), half)
            remote(r, r, k2_send.at[d * 2 + half], k2_recv.at[d * 2 + half], me.cousin(d)).wait_recv()
            forward(d, half).start()
    for d in range(8):
        for half in range(2):
            other = kvb.at[1 - me.core, pl.ds(pl.multiple_of(place(me.cousin(d).p[0], half) * 4, 4), 4), me.cousin(d).part]
            remote(other, other, f_send.at[d * 2 + half], f_recv.at[d * 2 + half], me.member(0, 1)).wait_recv()
    for d, dc in others:
        frm = me.member(d, dc)
        remote(qs.at[0], qr.at[frm.slot], q_send.at[d * 2 + dc], q_recv.at[frm.slot], frm).wait_recv()

    @pl.loop(0, 8)
    def _(i):
        for t in range(QW // 256):
            x = qr[2 * i + t // 2, pl.ds((t % 2) * 256, 256), :].astype(F32) * SCALE
            xt = x.T
            hi = xt.astype(BF16)
            lo = (xt - hi.astype(F32)).astype(BF16)
            for h in range(2):
                qT[i, 2 * t + h, 0:128, :] = hi[:, h * 128:(h + 1) * 128]
                qT[i, 2 * t + h, 128:256, :] = lo[:, h * 128:(h + 1) * 128]

    @pl.loop(0, 16)
    def _(b):
        for h in range(4):
            vT[b, h, 0:128, :] = kvb[1, b, h].T
            vT[b, h, 128:VR, :] = jnp.ones((VR - 128, 128), BF16)

    m_ref[...] = jnp.full_like(m_ref, NEG)
    acc_ref[...] = jnp.zeros_like(acc_ref)
    al[...] = jnp.zeros_like(al)
    for w in W[2:]:
        w[...] = jnp.zeros_like(w)

    i0 = me.pair_block

    def blk(j):
        return (i0 + j) % 8

    def source(i, bz):
        return Spot(me.p, (i // 4, (i // 2) % 2, bz), i % 2)

    def last_of(j):
        return source(blk(j), 0).sx

    def adv(u):
        j, b = u
        last = b == last_of(j)
        return jnp.minimum(jnp.where(last, j + 1, j), 7), jnp.where(last, 0, b + 1)

    def qk_stage(u, slot):
        j, b = u
        i = blk(j)
        for n in range(QW // CW):
            cols = pl.ds(n * CW, CW)
            kb = kvb[0, b].reshape(KB, 128)
            kk = jnp.concatenate([kb, kb], axis=1)
            qq = jnp.concatenate([qT[i, n * H + h] for h in range(H)], axis=1)
            s = jnp.dot(kk, qq, preferred_element_type=F32)
            S[slot][:, cols] = s
            mx[slot, :, cols] = jnp.max(s, axis=0, keepdims=True)

    def mask(u, slot):
        j, b = u

        @pl.loop(0, jnp.where(b == last_of(j), 1, 0))
        def _(_):
            here = source(blk(j), 0)
            ylo = (here.p[1] + here.b[1]) % 2
            row = lax.broadcasted_iota(jnp.int32, (KB, 128), 0)
            ky_hi = (row // 256 + ylo) % 2
            kpz, kbz = (row // 128) % 2, (row // 64) % 2
            key_at = (jnp.where(kbz == 0, kpz, 3 - kpz) * 2 + ky_hi) * 64 + row % 64
            for n in range(QW // 128):
                cols = pl.ds(n * 128, 128)
                col = lax.broadcasted_iota(jnp.int32, (KB, 128), 1) + (n % 4) * 128
                query_at = source(blk(j), n // 4).sy * 64 + col // 8
                s = jnp.where(key_at <= query_at, S[slot][:, cols], NEG)
                S[slot][:, cols] = s
                mx[slot, :, cols] = jnp.max(s, axis=0, keepdims=True)

    def soft_stage(u, slot):
        j, b = u
        m_old = jnp.where(b == 0, NEG, m_ref[...])
        m_new = jnp.maximum(m_old, mx[slot])
        m_ref[...] = m_new
        al[slot] = jnp.exp2(m_old - m_new)
        for n in range(QW // CW):
            cols = pl.ds(n * CW, CW)
            w = jnp.exp2(S[slot][:, cols] - m_new[:, n * CW:(n + 1) * CW]).astype(BF16)
            for h in range(H):
                W[slot][n * H + h] = w[:, h * 128:(h + 1) * 128]

    def pv_stage(u, slot):
        j, b = u
        par = j % 2
        for n in range(QW // CW):
            cols = pl.ds(n * CW, CW)
            ww = jnp.concatenate([W[slot][n * H + h] for h in range(H)], axis=1)
            vv = jnp.concatenate([vT[b, h] for h in range(4)], axis=1)
            acc_ref[par, :, cols] = acc_ref[par, :, cols] * al[slot, :, cols] + jnp.dot(vv, ww, preferred_element_type=F32)

    def outputs_to(s):
        to = Spot(me.p, (s // 8, (s // 4) % 2, s % 2), (s // 2) % 2)
        heads = pl.ds(pl.multiple_of(me.head_block * 8, 8), 8)
        return remote(ost.at[s], out_ref.at[:, heads, :], o_send.at[s], o_recv.at[me.head_block], to)

    def fin(u):
        j, b = u

        @pl.loop(0, jnp.where(b == last_of(j), 1, 0))
        def _(_):
            i = blk(j)
            par = j % 2
            o = acc_ref[par, 0:128, :] * (1.0 / acc_ref[par, 128:129, :])
            for bz in range(2):
                s = 2 * i + bz
                for t in range(2):
                    c0 = bz * 512 + t * 256
                    ost[s, pl.ds(t * 32, 32)] = o[:, c0:c0 + 256].T.reshape(32, 8, 128).astype(BF16)

                @pl.when(s != me.slot)
                def _():
                    outputs_to(s).start()

                @pl.when(s == me.slot)
                def _():
                    out_ref[:, pl.ds(pl.multiple_of(me.head_block * 8, 8), 8), :] = ost[s]

    z = jnp.int32(0)
    u0 = (z, z)
    u1 = adv(u0)
    qk_stage(u0, 0)
    qk_stage(u1, 1)
    mask(u0, 0)
    mask(u1, 1)

    def step(carry, cur, nxt):
        pa, pb, ca, cb, na, nb = carry
        qk_stage(na, nxt)
        qk_stage(nb, nxt + 1)
        soft_stage(ca, cur)
        soft_stage(cb, cur + 1)
        pv_stage(pa, nxt)
        pv_stage(pb, nxt + 1)
        mask(na, nxt)
        mask(nb, nxt + 1)
        fin(pa)
        fin(pb)
        n2 = adv(nb)
        return ca, cb, na, nb, n2, adv(n2)

    dummy = (z, jnp.where(last_of(z) == 0, 1, 0))
    u2 = adv(u1)
    carry = (dummy, dummy, u0, u1, u2, adv(u2))
    carry = lax.fori_loop(0, UNITS // 4, lambda _, c: step(step(c, 0, 2), 2, 0), carry)
    pv_stage(carry[0], 2)
    pv_stage(carry[1], 3)
    fin(carry[0])
    fin(carry[1])

    for d, dc in others:
        first(d, dc).wait_send()
        queries_to(d, dc).wait_send()
        frm = me.member(d, dc)
        outputs_to(frm.slot).wait_send()
        heads = pl.ds(pl.multiple_of(frm.head_block * 8, 8), 8)
        remote(ost.at[0], out_ref.at[:, heads, :], o_send.at[frm.slot], o_recv.at[frm.head_block], frm).wait_recv()
    for d in range(8):
        for half in range(2):
            forward(d, half).wait_send()
            if d:
                second(d, half).wait_send()


def shards(queries, keys, values):
    rows, heads, width = queries.shape
    start = lax.axis_index(("sx", "sy")) * rows
    positions = start + jnp.arange(rows, dtype=jnp.int32)
    angles = positions.astype(F32)[:, None] * frequencies(width)[None, :]
    cosine, sine = jnp.cos(angles), jnp.sin(angles)
    cos2 = jnp.concatenate([cosine, cosine], axis=1)
    sin2 = jnp.concatenate([-sine, sine], axis=1)
    wide = keys.astype(F32)
    turned = wide * cos2[:, None, :] + jnp.roll(wide, width // 2, axis=2) * sin2[:, None, :]
    kv = jnp.stack([turned.astype(BF16).transpose(1, 0, 2), values.transpose(1, 0, 2)])

    def eightfold(a):
        return jnp.broadcast_to(a[:, None, :], (rows, 8, width)).reshape(rows * 8, width)

    dma = pltpu.SemaphoreType.DMA
    return pl.pallas_call(
        kernel,
        out_shape=jax.ShapeDtypeStruct((rows, heads, width), BF16),
        in_specs=[pl.BlockSpec(memory_space=pltpu.VMEM)] * 4,
        out_specs=pl.BlockSpec(memory_space=pltpu.VMEM),
        scratch_shapes=[
            pltpu.VMEM((16, 512, 128), BF16),
            pltpu.VMEM((16, 512, 128), BF16),
            pltpu.VMEM((2, 16, 4, 128, 128), BF16),
            pltpu.VMEM((16, 64, 8, 128), BF16),
            pltpu.VMEM((8, 8, 256, 128), BF16),
            pltpu.VMEM((16, 4, VR, 128), BF16),
            *[pltpu.VMEM((KB, QW), F32)] * 4,
            *[pltpu.VMEM((8, KB, 128), BF16)] * 4,
            pltpu.VMEM((4, 1, QW), F32),
            pltpu.VMEM((4, 1, QW), F32),
            pltpu.VMEM((1, QW), F32),
            pltpu.VMEM((2, VR, QW), F32),
            *[dma((16,))] * 10,
        ],
        compiler_params=pltpu.CompilerParams(
            collective_id=0, has_side_effects=True, vmem_limit_bytes=58 << 20
        ),
        name="fused",
    )(queries, kv, eightfold(cos2), eightfold(sin2))


def solution(mesh):
    placed = P(("sx", "sy"), None, None)
    return jax.shard_map(
        shards, mesh=mesh, in_specs=(placed, placed, placed), out_specs=placed, check_vma=False
    )
```

```python
import functools
import math

import jax
import jax.numpy as jnp
from jax import lax
from jax.experimental import pallas as pl
from jax.experimental.pallas import tpu as pltpu
from jax.sharding import PartitionSpec as P

MESH = pl.DeviceIdType.MESH
F32 = jnp.float32
BF16 = jnp.bfloat16
NEG = -1e30
CW = 256
QW = 1024
KB = 512
VR = 144
SCALE = math.log2(math.e) / math.sqrt(128.0)


def frequencies(head_width):
    half_index = jnp.arange(head_width // 2, dtype=F32)
    base_rate = jnp.power(F32(500000.0), -2.0 * half_index / head_width)
    wavelen = 2.0 * math.pi / base_rate
    smooth = (8192.0 / wavelen - 1.0) / 3.0
    blended = (1.0 - smooth) * base_rate / 8.0 + smooth * base_rate
    return jnp.where(
        wavelen < 2048.0, base_rate, jnp.where(wavelen > 8192.0, base_rate / 8.0, blended)
    )


def place(p, b):
    return p ^ (3 * b)


class Spot:
    def __init__(self, p, b, core):
        self.p, self.b, self.core = tuple(p), tuple(b), core

    @staticmethod
    def own():
        sx, sy = lax.axis_index("sx"), lax.axis_index("sy")
        xyz = (sx >> 2, (sy & 1) * 2 + ((sx >> 1) & 1), sy >> 1)
        return Spot([((c + 1) >> 1) & 1 for c in xyz], [c >> 1 for c in xyz], sx & 1)

    @property
    def sx(self):
        ylo = self.p[1] ^ self.b[1]
        return place(self.p[0], self.b[0]) * 4 + ylo * 2 + self.core

    @property
    def sy(self):
        return place(self.p[2], self.b[2]) * 2 + self.b[1]

    @property
    def device(self):
        return (self.sx, self.sy)

    @property
    def chip(self):
        return self.b[0] * 4 + self.b[1] * 2 + self.b[2]

    @property
    def head_block(self):
        return self.chip * 2 + self.core

    @property
    def pair_block(self):
        return (self.b[0] * 2 + self.b[1]) * 2 + self.core

    @property
    def slot(self):
        return self.pair_block * 2 + self.b[2]

    @property
    def part(self):
        return self.p[1] * 2 + self.p[2]

    def member(self, d, dc):
        return Spot(self.p, [b ^ ((d >> s) & 1) for b, s in zip(self.b, (2, 1, 0))], self.core ^ dc)

    def cousin(self, d):
        return Spot([p ^ ((d >> s) & 1) for p, s in zip(self.p, (2, 1, 0))], self.b, self.core)


ORDER = (0, 7, 6, 1, 5, 2, 4, 3)
RELAYS = tuple((0, half, e) for e in (1, 2, 4) for half in range(2)) + (
    (2, 0, 1), (1, 1, 2), (1, 0, 4), (2, 1, 4), (4, 1, 1), (4, 0, 2), (3, 0, 4), (5, 1, 2))


def kernel(q_ref, kv_ref, cos_ref, sin_ref, out_ref,
           qs, qr, kvb, ost, k2, vT, key_place, s0, s1, s2, s3, p0, p1, p2, p3, mx, al, m_ref, acc_ref,
           q_send, q_recv, k1_send, k1_recv, k2_send, k2_recv, f_send, f_recv, o_send, o_recv):
    S, W = (s0, s1, s2, s3), (p0, p1, p2, p3)
    H = CW // 128
    me = Spot.own()
    others = [(d, dc) for d in ORDER for dc in (1, 0) if (d, dc) != (0, 0)]

    def remote(src, dst, send, recv, spot):
        return pltpu.make_async_remote_copy(src_ref=src, dst_ref=dst, send_sem=send, recv_sem=recv, device_id=spot.device, device_id_type=MESH)

    barrier = pltpu.get_barrier_semaphore()
    for d, dc in others:
        pl.semaphore_signal(barrier, inc=1, device_id=me.member(d, dc).device, device_id_type=MESH)
    for d in range(1, 8):
        pl.semaphore_signal(barrier, inc=1, device_id=me.cousin(d).device, device_id_type=MESH)
    pl.semaphore_wait(barrier, len(others) + 7)

    def kv_spot(role, src):
        return kvb.at[role, src.sx, src.part, pl.ds(pl.multiple_of(src.b[2] * 64, 64), 64), :]

    def first(d, dc):
        to = me.member(d, dc)
        return remote(kv_ref.at[to.core, to.chip], kv_spot(to.core, me), k1_send.at[d * 2 + dc], k1_recv.at[me.slot], to)

    for d, dc in others:
        first(d, dc).start()
    kvb[me.core, me.sx, me.part, pl.ds(pl.multiple_of(me.b[2] * 64, 64), 64), :] = kv_ref[me.core, me.chip]

    def queries_to(d, dc):
        to = me.member(d, dc)
        return remote(qs.at[to.head_block], qr.at[me.slot], q_send.at[d * 2 + dc], q_recv.at[me.slot], to)

    for d in ORDER:
        to = me.member(d, 0)
        x = q_ref[:, pl.ds(pl.multiple_of(to.chip * 16, 16), 16), :].astype(F32)
        for c in range(2):
            part = x[:, c * 8:(c + 1) * 8, :].reshape(512, 128)
            turned = part * cos_ref[...] + pltpu.roll(part, 64, 1) * sin_ref[...]
            flat = turned.astype(BF16).T
            for h in range(4):
                qs[to.chip * 2 + c, h] = flat[:, h * 128:(h + 1) * 128]
        for dc in (1, 0):
            if (d, dc) != (0, 0):
                queries_to(d, dc).start()
    qr[me.slot] = qs[me.head_block]

    for d, dc in others:
        frm = me.member(d, dc)
        remote(kv_ref.at[0, 0], kv_spot(me.core, frm), k1_send.at[d * 2 + dc], k1_recv.at[frm.slot], frm).wait_recv()

    def region(spot, half):
        return kvb.at[me.core, pl.ds(pl.multiple_of(place(spot.p[0], half) * 4, 4), 4), spot.part]

    def relay(a, half, e):
        r = region(me.cousin(a), half)
        n = (a ^ e) * 2 + half
        return remote(r, r, k2_send.at[n], k2_recv.at[n], me.cousin(e))

    def forward(d, half):
        r = region(me.cousin(d), half)
        return remote(r, r, f_send.at[d * 2 + half], f_recv.at[d * 2 + half], me.member(0, 1))

    def arrived(d, half):
        r = region(me.cousin(d), half)
        return remote(r, r, k2_send.at[d * 2 + half], k2_recv.at[d * 2 + half], me.cousin(d))

    def handed(d, half):
        r = kvb.at[1 - me.core, pl.ds(pl.multiple_of(place(me.cousin(d).p[0], half) * 4, 4), 4), me.cousin(d).part]
        return remote(r, r, f_send.at[d * 2 + half], f_recv.at[d * 2 + half], me.member(0, 1))

    def pass_on(d):
        for half in range(2):
            arrived(d, half).wait_recv()
            forward(d, half).start()

    for d in (1, 2, 4):
        for half in range(2):
            relay(0, half, d).start()
    for half in range(2):
        forward(0, half).start()

    row = lax.broadcasted_iota(jnp.int32, (KB, 128), 0)
    for ylo in range(2):
        z_at = ((row >> 7) & 1) ^ (3 * ((row >> 6) & 1))
        key_place[ylo] = (z_at * 2 + ((row >> 8) ^ ylo)) * 64 + (row & 63)

    acc_ref[...] = jnp.zeros_like(acc_ref)
    al[...] = jnp.zeros_like(al)
    for w in W[2:]:
        w[...] = jnp.zeros_like(w)

    @pl.loop(0, 16)
    def _(b):
        for h in range(4):
            vT[b, h, 128:VR, :] = jnp.ones((VR - 128, 128), BF16)

    for d in (1, 2):
        pass_on(d)
    for relayed in ((2, 0, 1), (1, 1, 2), (1, 0, 4), (2, 1, 4)):
        relay(*relayed).start()
    pass_on(4)
    for relayed in ((4, 1, 1), (4, 0, 2)):
        relay(*relayed).start()
    pass_on(3)
    relay(3, 0, 4).start()
    for d in range(4):
        for half in range(2):
            handed(d, half).wait_recv()

    px = me.p[0]

    def values_of(half_of):
        @pl.loop(0, 4)
        def _(t):
            b = half_of * 4 + t
            for h in range(4):
                vT[b, h, 0:128, :] = kvb[1, b, h].T
                wide = kvb[0, b, h].astype(F32) * SCALE
                hi = wide.astype(BF16)
                k2[b, 0, pl.ds(h * 128, 128), :] = hi
                k2[b, 1, pl.ds(h * 128, 128), :] = (wide - hi.astype(F32)).astype(BF16)

    values_of(place(px, 0))
    values_of(place(px, 1))

    own_block = me.pair_block

    def early_block(k):
        g = k >> 1
        return own_block ^ (((g + 1) >> 1 & 1) * 4 + (g & 1) * 2 + (k & 1))

    def source(i, bz):
        return Spot(me.p, (i >> 2, (i >> 1) & 1, bz), i & 1)

    def rank(i):
        return (i & 4) + ((me.p[1] ^ ((i >> 1) & 1)) * 2) + (i & 1)

    def early(k, r):
        i = early_block(k)
        b = (px ^ (3 * (r >> 2))) * 4 + (r & 3)
        end = jnp.where(r == rank(i), 1, 0)
        done = end * (1 - (px | (i >> 2)))
        return i + 8 * b + 128 * jnp.where(r == 0, 1, 0) + 256 * done + 512 * end

    def next_early(k, r):
        end = r == rank(early_block(k))
        return jnp.where(end, k + 1, k), jnp.where(end, 0, r + 1)

    def late(v):
        r0, r1 = v & 7, v & 3
        i0 = 4 | ((own_block & 3) ^ (3 - (v >> 3)))
        i1 = early_block(7 - (v >> 2))
        u0 = i0 + 8 * (r0 + 4) + 256 * jnp.where(r0 == 7, 1, 0)
        u1 = i1 + 8 * r1 + 256 * jnp.where(r1 == 3, 1, 0)
        return jnp.where(px == 0, u0, u1)

    def qblock(u):
        return u & 7

    def kblock(u):
        return (u >> 3) & 15

    def queries_in(u):
        @pl.loop(0, (u >> 7) & 1)
        def _(_):
            i = qblock(u)
            for bz in range(2):
                s = 2 * i + bz

                @pl.when(s != me.slot)
                def _():
                    remote(qs.at[0], qr.at[s], q_send.at[0], q_recv.at[s], me.member(1, 0)).wait_recv()

    def qk_stage(u, slot):
        i, b = qblock(u), kblock(u)
        for n in range(QW // CW):
            cols = pl.ds(n * CW, CW)
            kk = jnp.concatenate([k2[b, 0], k2[b, 1]], axis=1)
            qq = jnp.concatenate([qr[2 * i + (n * H + h) // 4, (n * H + h) % 4] for h in range(H)], axis=1)
            qq = jnp.concatenate([qq, qq], axis=0)
            s = jnp.dot(kk, qq, preferred_element_type=F32)
            S[slot][:, cols] = s
            mx[slot, :, cols] = jnp.max(s, axis=0, keepdims=True)

    def mask(u, slot):
        @pl.loop(0, u >> 9)
        def _(_):
            here = source(qblock(u), 0)
            key_at = key_place[me.p[1] ^ here.b[1]]
            lane = lax.broadcasted_iota(jnp.int32, (1, 128), 1) >> 3
            for n in range(QW // 128):
                cols = pl.ds(n * 128, 128)
                query_at = lane + (source(qblock(u), n // 4).sy * 64 + n % 4 * 16)
                s = jnp.where(key_at <= query_at, S[slot][:, cols], NEG)
                S[slot][:, cols] = s
                mx[slot, :, cols] = jnp.max(s, axis=0, keepdims=True)

    def soft_stage(u, slot):
        i = qblock(u)
        m_old = jnp.where((u >> 7) & 1 == 1, NEG, m_ref[i])
        m_new = jnp.maximum(m_old, mx[slot])
        m_ref[i] = m_new
        al[slot] = jnp.exp2(m_old - m_new)
        for n in range(QW // CW):
            cols = pl.ds(n * CW, CW)
            w = jnp.exp2(S[slot][:, cols] - m_new[:, n * CW:(n + 1) * CW]).astype(BF16)
            for h in range(H):
                W[slot][n * H + h] = w[:, h * 128:(h + 1) * 128]

    def pv_stage(u, slot):
        i, b = qblock(u), kblock(u)
        for n in range(QW // CW):
            cols = pl.ds(n * CW, CW)
            ww = jnp.concatenate([W[slot][n * H + h] for h in range(H)], axis=1)
            vv = jnp.concatenate([vT[b, h] for h in range(4)], axis=1)
            acc_ref[i, :, cols] = acc_ref[i, :, cols] * al[slot, :, cols] + jnp.dot(vv, ww, preferred_element_type=F32)

    def outputs_to(s):
        to = Spot(me.p, (s >> 3, (s >> 2) & 1, s & 1), (s >> 1) & 1)
        heads = pl.ds(pl.multiple_of(me.head_block * 8, 8), 8)
        return remote(ost.at[s], out_ref.at[:, heads, :], o_send.at[s], o_recv.at[me.head_block], to)

    def fin(u):
        @pl.loop(0, (u >> 8) & 1)
        def _(_):
            i = qblock(u)
            o = acc_ref[i, 0:128, :] * (1.0 / acc_ref[i, 128:129, :])
            for bz in range(2):
                s = 2 * i + bz
                for t in range(2):
                    c0 = bz * 512 + t * 256
                    ost[s, pl.ds(t * 32, 32)] = o[:, c0:c0 + 256].T.reshape(32, 8, 128).astype(BF16)

                @pl.when(s != me.slot)
                def _():
                    outputs_to(s).start()

                @pl.when(s == me.slot)
                def _():
                    out_ref[:, pl.ds(pl.multiple_of(me.head_block * 8, 8), 8), :] = ost[s]

    def step(old, now, new, cur, nxt):
        if new is not None:
            for n in range(2):
                queries_in(new[n])
            for n in range(2):
                qk_stage(new[n], nxt + n)
        for n in range(2):
            soft_stage(now[n], cur + n)
        for n in range(2):
            pv_stage(old[n], nxt + n)
        if new is not None:
            for n in range(2):
                mask(new[n], nxt + n)
        for n in range(2):
            fin(old[n])

    def take(at):
        k, r = at
        k1, r1 = next_early(k, r)
        return (early(k, r), early(k1, r1)), next_early(k1, r1)

    z = jnp.int32(0)
    u01, at = take((z, z))
    for n in range(2):
        queries_in(u01[n])
        qk_stage(u01[n], n)
        mask(u01[n], n)

    dummy = (u01[0] & 127,) * 2

    def early_steps(t, carry):
        old, now, at = carry
        @pl.loop(0, jnp.where(t == 1, 1, 0))
        def _(_):
            pass_on(5)
            relay(5, 1, 2).start()
            pass_on(6)

        @pl.loop(0, jnp.where(t == 4, 1, 0))
        def _(_):
            pass_on(7)

        new, at = take(at)
        step(old, now, new, 0, 2)
        new2, at = take(at)
        step(now, new, new2, 2, 0)
        return new, new2, at

    old, now, at = lax.fori_loop(0, 8, early_steps, (dummy, u01, at))
    new, _ = take(at)
    step(old, now, new, 0, 2)
    old, now = now, new

    for d in range(4, 8):
        for half in range(2):
            handed(d, half).wait_recv()
    values_of(place(1 - px, 0))
    values_of(place(1 - px, 1))

    def late_steps(t, carry):
        old, now = carry
        new = late(4 * t), late(4 * t + 1)
        step(old, now, new, 2, 0)
        new2 = late(4 * t + 2), late(4 * t + 3)
        step(now, new, new2, 0, 2)
        return new, new2

    old, now = lax.fori_loop(0, 8, late_steps, (old, now))
    step(old, now, None, 2, 0)
    for n in range(2):
        pv_stage(now[n], 2 + n)
    for n in range(2):
        fin(now[n])

    for d, dc in others:
        first(d, dc).wait_send()
        queries_to(d, dc).wait_send()
        frm = me.member(d, dc)
        outputs_to(frm.slot).wait_send()
        heads = pl.ds(pl.multiple_of(frm.head_block * 8, 8), 8)
        remote(ost.at[0], out_ref.at[:, heads, :], o_send.at[frm.slot], o_recv.at[frm.head_block], frm).wait_recv()
    for d in range(8):
        for half in range(2):
            forward(d, half).wait_send()
    for relayed in RELAYS:
        relay(*relayed).wait_send()


def shards(queries, keys, values):
    rows, heads, width = queries.shape
    start = lax.axis_index(("sx", "sy")) * rows
    positions = start + jnp.arange(rows, dtype=jnp.int32)
    angles = positions.astype(F32)[:, None] * frequencies(width)[None, :]
    cosine, sine = jnp.cos(angles), jnp.sin(angles)
    cos2 = jnp.concatenate([cosine, cosine], axis=1)
    sin2 = jnp.concatenate([-sine, sine], axis=1)
    wide = keys.astype(F32)
    turned = wide * cos2[:, None, :] + jnp.roll(wide, width // 2, axis=2) * sin2[:, None, :]
    kv = jnp.stack([turned.astype(BF16).transpose(1, 0, 2), values.transpose(1, 0, 2)])

    def eightfold(a):
        return jnp.broadcast_to(a[:, None, :], (rows, 8, width)).reshape(rows * 8, width)

    dma = pltpu.SemaphoreType.DMA
    return pl.pallas_call(
        kernel,
        out_shape=jax.ShapeDtypeStruct((rows, heads, width), BF16),
        in_specs=[pl.BlockSpec(memory_space=pltpu.VMEM)] * 4,
        out_specs=pl.BlockSpec(memory_space=pltpu.VMEM),
        scratch_shapes=[
            pltpu.VMEM((16, 4, 128, 128), BF16),
            pltpu.VMEM((16, 4, 128, 128), BF16),
            pltpu.VMEM((2, 16, 4, 128, 128), BF16),
            pltpu.VMEM((16, 64, 8, 128), BF16),
            pltpu.VMEM((16, 2, KB, 128), BF16),
            pltpu.VMEM((16, 4, VR, 128), BF16),
            pltpu.VMEM((2, KB, 128), jnp.int32),
            *[pltpu.VMEM((KB, QW), F32)] * 4,
            *[pltpu.VMEM((8, KB, 128), BF16)] * 4,
            pltpu.VMEM((4, 1, QW), F32),
            pltpu.VMEM((4, 1, QW), F32),
            pltpu.VMEM((8, 1, QW), F32),
            pltpu.VMEM((8, VR, QW), F32),
            *[dma((16,))] * 10,
        ],
        compiler_params=pltpu.CompilerParams(
            collective_id=0, has_side_effects=True, vmem_limit_bytes=40 << 20
        ),
        name="fused",
    )(queries, kv, eightfold(cos2), eightfold(sin2))


def solution(mesh):
    placed = P(("sx", "sy"), None, None)
    return jax.shard_map(
        shards, mesh=mesh, in_specs=(placed, placed, placed), out_specs=placed, check_vma=False
    )
```

```python
import functools
import math

import jax
import jax.numpy as jnp
from jax import lax
from jax.experimental import pallas as pl
from jax.experimental.pallas import tpu as pltpu
from jax.sharding import PartitionSpec as P

MESH = pl.DeviceIdType.MESH
F32 = jnp.float32
BF16 = jnp.bfloat16
NEG = -1e30
CW = 256
QW = 1024
KB = 512
VR = 144
SCALE = math.log2(math.e) / math.sqrt(128.0)


def frequencies(head_width):
    half_index = jnp.arange(head_width // 2, dtype=F32)
    base_rate = jnp.power(F32(500000.0), -2.0 * half_index / head_width)
    wavelen = 2.0 * math.pi / base_rate
    smooth = (8192.0 / wavelen - 1.0) / 3.0
    blended = (1.0 - smooth) * base_rate / 8.0 + smooth * base_rate
    return jnp.where(
        wavelen < 2048.0, base_rate, jnp.where(wavelen > 8192.0, base_rate / 8.0, blended)
    )


def place(p, b):
    return p ^ (3 * b)


class Spot:
    def __init__(self, p, b, core):
        self.p, self.b, self.core = tuple(p), tuple(b), core

    @staticmethod
    def own():
        sx, sy = lax.axis_index("sx"), lax.axis_index("sy")
        xyz = (sx >> 2, (sy & 1) * 2 + ((sx >> 1) & 1), sy >> 1)
        return Spot([((c + 1) >> 1) & 1 for c in xyz], [c >> 1 for c in xyz], sx & 1)

    @property
    def sx(self):
        ylo = self.p[1] ^ self.b[1]
        return place(self.p[0], self.b[0]) * 4 + ylo * 2 + self.core

    @property
    def sy(self):
        return place(self.p[2], self.b[2]) * 2 + self.b[1]

    @property
    def device(self):
        return (self.sx, self.sy)

    @property
    def chip(self):
        return self.b[0] * 4 + self.b[1] * 2 + self.b[2]

    @property
    def head_block(self):
        return self.chip * 2 + self.core

    @property
    def pair_block(self):
        return (self.b[0] * 2 + self.b[1]) * 2 + self.core

    @property
    def slot(self):
        return self.pair_block * 2 + self.b[2]

    @property
    def part(self):
        return self.p[1] * 2 + self.p[2]

    def member(self, d, dc):
        return Spot(self.p, [b ^ ((d >> s) & 1) for b, s in zip(self.b, (2, 1, 0))], self.core ^ dc)

    def cousin(self, d):
        return Spot([p ^ ((d >> s) & 1) for p, s in zip(self.p, (2, 1, 0))], self.b, self.core)


ORDER = (7, 6, 1, 0, 4, 3, 5, 2)
HEAD_RUNS = 3
RELAYS = tuple((0, half, e) for e in (1, 2, 4) for half in range(2)) + (
    (2, 0, 1), (1, 1, 2), (1, 0, 4), (2, 1, 4), (4, 1, 1), (4, 0, 2), (3, 0, 4), (5, 1, 2))


def kernel(q_ref, k_ref, v_ref, cos_ref, sin_ref, out_ref,
           flat_kv, kv_ref, qs, qr, kvb, ost, k2, vT, key_place, s0, s1, s2, s3, p0, p1, p2, p3, mx, al, m_ref, acc_ref,
           q_send, q_recv, k1_send, k1_recv, k2_send, k2_recv, f_send, f_recv, o_send, o_recv):
    S, W = (s0, s1, s2, s3), (p0, p1, p2, p3)
    H = CW // 128
    me = Spot.own()
    others = [(d, dc) for d in ORDER for dc in (1, 0) if (d, dc) != (0, 0)]

    def remote(src, dst, send, recv, spot):
        return pltpu.make_async_remote_copy(src_ref=src, dst_ref=dst, send_sem=send, recv_sem=recv, device_id=spot.device, device_id_type=MESH)

    barrier = pltpu.get_barrier_semaphore()
    for d, dc in others:
        pl.semaphore_signal(barrier, inc=1, device_id=me.member(d, dc).device, device_id_type=MESH)
    for d in range(1, 8):
        pl.semaphore_signal(barrier, inc=1, device_id=me.cousin(d).device, device_id_type=MESH)

    k = k_ref[...].astype(F32).reshape(512, 128)
    flat_kv[0] = k * cos_ref[...] + pltpu.roll(k, 64, 1) * sin_ref[...]
    flat_kv[1] = v_ref[...].astype(F32).reshape(512, 128)
    for role in range(2):
        for h in range(8):
            kv_ref[role, h] = flat_kv[role, pl.ds(h, 64, stride=8), :].astype(BF16)

    pl.semaphore_wait(barrier, len(others) + 7)

    def kv_spot(role, src):
        return kvb.at[role, src.sx, src.part, pl.ds(pl.multiple_of(src.b[2] * 64, 64), 64), :]

    def first(d, dc):
        to = me.member(d, dc)
        return remote(kv_ref.at[to.core, to.chip], kv_spot(to.core, me), k1_send.at[d * 2 + dc], k1_recv.at[me.slot], to)

    for d, dc in others:
        first(d, dc).start()
    kvb[me.core, me.sx, me.part, pl.ds(pl.multiple_of(me.b[2] * 64, 64), 64), :] = kv_ref[me.core, me.chip]

    def queries_to(d, dc):
        to = me.member(d, dc)
        return remote(qs.at[to.head_block], qr.at[me.slot], q_send.at[d * 2 + dc], q_recv.at[me.slot], to)

    for d in ORDER:
        to = me.member(d, 0)
        x = q_ref[:, pl.ds(pl.multiple_of(to.chip * 16, 16), 16), :].astype(F32)
        for c in range(2):
            part = x[:, c * 8:(c + 1) * 8, :].reshape(512, 128)
            turned = part * cos_ref[...] + pltpu.roll(part, 64, 1) * sin_ref[...]
            flat = turned.astype(BF16).T
            for h in range(4):
                qs[to.chip * 2 + c, h] = flat[:, h * 128:(h + 1) * 128]
        for dc in (1, 0):
            if (d, dc) != (0, 0):
                queries_to(d, dc).start()
    qr[me.slot] = qs[me.head_block]

    for d, dc in others:
        frm = me.member(d, dc)
        remote(kv_ref.at[0, 0], kv_spot(me.core, frm), k1_send.at[d * 2 + dc], k1_recv.at[frm.slot], frm).wait_recv()

    def region(spot, half):
        return kvb.at[me.core, pl.ds(pl.multiple_of(place(spot.p[0], half) * 4, 4), 4), spot.part]

    def relay(a, half, e):
        r = region(me.cousin(a), half)
        n = (a ^ e) * 2 + half
        return remote(r, r, k2_send.at[n], k2_recv.at[n], me.cousin(e))

    def forward(d, half):
        r = region(me.cousin(d), half)
        return remote(r, r, f_send.at[d * 2 + half], f_recv.at[d * 2 + half], me.member(0, 1))

    def arrived(d, half):
        r = region(me.cousin(d), half)
        return remote(r, r, k2_send.at[d * 2 + half], k2_recv.at[d * 2 + half], me.cousin(d))

    def handed(d, half):
        r = kvb.at[1 - me.core, pl.ds(pl.multiple_of(place(me.cousin(d).p[0], half) * 4, 4), 4), me.cousin(d).part]
        return remote(r, r, f_send.at[d * 2 + half], f_recv.at[d * 2 + half], me.member(0, 1))

    def pass_on(d, half, *axes):
        arrived(d, half).wait_recv()
        for e in axes:
            relay(d, half, e).start()
        forward(d, half).start()

    for e, half in ((1, 1), (2, 0), (4, 1), (1, 0), (2, 1), (4, 0)):
        relay(0, half, e).start()
    for half in range(2):
        forward(0, half).start()

    row = lax.broadcasted_iota(jnp.int32, (KB, 128), 0)
    for ylo in range(2):
        z_at = ((row >> 7) & 1) ^ (3 * ((row >> 6) & 1))
        key_place[ylo] = (z_at * 2 + ((row >> 8) ^ ylo)) * 64 + (row & 63)

    acc_ref[...] = jnp.zeros_like(acc_ref)
    al[...] = jnp.zeros_like(al)
    for w in W[2:]:
        w[...] = jnp.zeros_like(w)

    @pl.loop(0, 16)
    def _(b):
        for h in range(4):
            vT[b, h, 128:VR, :] = jnp.ones((VR - 128, 128), BF16)

    pass_on(2, 0, 1)
    pass_on(1, 1, 2)
    pass_on(1, 0, 4)
    pass_on(2, 1, 4)
    pass_on(4, 1, 1)
    pass_on(4, 0, 2)
    pass_on(3, 0, 4)
    pass_on(3, 1)
    for d in range(4):
        for half in range(2):
            handed(d, half).wait_recv()

    px = me.p[0]

    def keys_of(half_of):
        @pl.loop(0, 4)
        def _(t):
            b = half_of * 4 + t
            for h in range(4):
                vT[b, h, 0:128, :] = kvb[1, b, h].T
                wide = kvb[0, b, h].astype(F32) * SCALE
                hi = wide.astype(BF16)
                k2[b, 0, pl.ds(h * 128, 128), :] = hi
                k2[b, 1, pl.ds(h * 128, 128), :] = (wide - hi.astype(F32)).astype(BF16)

    keys_of(place(px, 0))
    keys_of(place(px, 1))

    own_block = me.pair_block

    def early_block(k):
        g = k >> 1
        return own_block ^ ((1 - (g & 1)) * 4 + (1 - (g >> 1)) * 2 + (k & 1))

    def source(i, bz):
        return Spot(me.p, (i >> 2, (i >> 1) & 1, bz), i & 1)

    def rank(i):
        return (i & 4) + ((me.p[1] ^ ((i >> 1) & 1)) * 2) + (i & 1)

    def run(n):
        k = jnp.where(n < HEAD_RUNS, n, jnp.where(n < 2 * HEAD_RUNS, n - HEAD_RUNS, n >> 1))
        side = jnp.where(n < HEAD_RUNS, 0, jnp.where(n < 2 * HEAD_RUNS, 1, n & 1))
        return early_block(k), side

    def length(n):
        i, side = run(n)
        return jnp.where(side == 0, rank(i) + 1, jnp.where(px == 0, (i & 4) * 2, 4))

    def unit(at):
        n, r, seen = at
        i, side = run(n)
        mine = (px ^ (3 * (r >> 2))) * 4 + (r & 3)
        other = r + 4 * (1 - px)
        end = jnp.where(r + 1 == length(n), 1, 0)
        far = jnp.where(side == 1, 1, 0)
        done = end * jnp.where(far + (1 - (px | (i >> 2))) > 0, 1, 0)
        first_of = jnp.where(r == 0, 1, 0) * (1 - far)
        code = i + 8 * jnp.where(side == 0, mine, other) + 128 * first_of + 256 * done + 512 * end * (1 - far) + 1024 * far * (1 - seen)
        n1 = n + 1
        n1 = jnp.where(length(n1) == 0, n1 + 1, n1)
        n1 = jnp.where(length(n1) == 0, n1 + 1, n1)
        after = jnp.where(end == 1, jnp.minimum(n1, 15), n), jnp.where(end == 1, 0, r + 1), seen | far
        return code, after

    def qblock(u):
        return u & 7

    def kblock(u):
        return (u >> 3) & 15

    def queries_in(u):
        @pl.loop(0, (u >> 7) & 1)
        def _(_):
            i = qblock(u)
            for bz in range(2):
                s = 2 * i + bz

                @pl.when(s != me.slot)
                def _():
                    remote(qs.at[0], qr.at[s], q_send.at[0], q_recv.at[s], me.member(1, 0)).wait_recv()

    def qk_stage(u, slot, pieces=range(QW // CW)):
        i, b = qblock(u), kblock(u)
        for n in pieces:
            cols = pl.ds(n * CW, CW)
            kk = jnp.concatenate([k2[b, 0], k2[b, 1]], axis=1)
            qq = jnp.concatenate([qr[2 * i + (n * H + h) // 4, (n * H + h) % 4] for h in range(H)], axis=1)
            qq = jnp.concatenate([qq, qq], axis=0)
            s = jnp.dot(kk, qq, preferred_element_type=F32)
            S[slot][:, cols] = s
            mx[slot, :, cols] = jnp.max(s, axis=0, keepdims=True)

    def mask(u, slot):
        @pl.loop(0, (u >> 9) & 1)
        def _(_):
            here = source(qblock(u), 0)
            key_at = key_place[me.p[1] ^ here.b[1]]
            lane = lax.broadcasted_iota(jnp.int32, (1, 128), 1) >> 3
            for n in range(QW // 128):
                cols = pl.ds(n * 128, 128)
                query_at = lane + (source(qblock(u), n // 4).sy * 64 + n % 4 * 16)
                s = jnp.where(key_at <= query_at, S[slot][:, cols], NEG)
                S[slot][:, cols] = s
                mx[slot, :, cols] = jnp.max(s, axis=0, keepdims=True)

    def soft_stage(u, slot, pieces=range(QW // CW)):
        i = qblock(u)
        for n in pieces:
            cols = pl.ds(n * CW, CW)
            m_old = jnp.where((u >> 7) & 1 == 1, NEG, m_ref[i, :, cols])
            m_new = jnp.maximum(m_old, mx[slot, :, cols])
            m_ref[i, :, cols] = m_new
            al[slot, :, cols] = jnp.exp2(m_old - m_new)
            w = jnp.exp2(S[slot][:, cols] - m_new).astype(BF16)
            for h in range(H):
                W[slot][n * H + h] = w[:, h * 128:(h + 1) * 128]

    def pv_stage(u, slot):
        i, b = qblock(u), kblock(u)
        for n in range(QW // CW):
            cols = pl.ds(n * CW, CW)
            ww = jnp.concatenate([W[slot][n * H + h] for h in range(H)], axis=1)
            vv = jnp.concatenate([vT[b, h] for h in range(4)], axis=1)
            acc_ref[i, :, cols] = acc_ref[i, :, cols] * al[slot, :, cols] + jnp.dot(vv, ww, preferred_element_type=F32)

    def outputs_to(s):
        to = Spot(me.p, (s >> 3, (s >> 2) & 1, s & 1), (s >> 1) & 1)
        heads = pl.ds(pl.multiple_of(me.head_block * 8, 8), 8)
        return remote(ost.at[s], out_ref.at[:, heads, :], o_send.at[s], o_recv.at[me.head_block], to)

    def fin(u):
        @pl.loop(0, (u >> 8) & 1)
        def _(_):
            i = qblock(u)
            o = acc_ref[i, 0:128, :] * (1.0 / acc_ref[i, 128:129, :])
            for bz in range(2):
                s = 2 * i + bz
                for t in range(2):
                    c0 = bz * 512 + t * 256
                    ost[s, pl.ds(t * 32, 32)] = o[:, c0:c0 + 256].T.reshape(32, 8, 128).astype(BF16)

                @pl.when(s != me.slot)
                def _():
                    outputs_to(s).start()

                @pl.when(s == me.slot)
                def _():
                    out_ref[:, pl.ds(pl.multiple_of(me.head_block * 8, 8), 8), :] = ost[s]

    def other_keys(u):
        @pl.loop(0, (u >> 10) & 1)
        def _(_):
            pass_on(7, 0)
            pass_on(7, 1)
            for d in range(4, 8):
                for half in range(2):
                    handed(d, half).wait_recv()
            keys_of(place(1 - px, 0))
            keys_of(place(1 - px, 1))

    def any_of(bits, units):
        got = units[0] | units[1]
        return jnp.where((got & bits) != 0, 1, 0)

    def step(old, now, new, at, cur, nxt):
        if new is None:
            for n in range(2):
                soft_stage(now[n], cur + n)
            for n in range(2):
                pv_stage(old[n], nxt + n)
            for n in range(2):
                fin(old[n])
            return None

        @pl.loop(0, any_of(128 + 1024, new))
        def _(_):
            for n in range(2):
                queries_in(new[n])
                other_keys(new[n])

        ahead, at = take(at)
        for n in range(2):
            for piece in range(QW // CW):
                qk_stage(new[n], nxt + n, (piece,))
                soft_stage(now[n], cur + n, (piece,))
        for n in range(2):
            pv_stage(old[n], nxt + n)

        @pl.loop(0, jnp.maximum(any_of(512, new), any_of(256, old)))
        def _(_):
            for n in range(2):
                mask(new[n], nxt + n)
            for n in range(2):
                fin(old[n])

        return ahead, at

    def take(at):
        u, at = unit(at)
        v, at = unit(at)
        return (u, v), at

    z = jnp.int32(0)
    u01, at = take((z, z, z))
    for n in range(2):
        queries_in(u01[n])
        qk_stage(u01[n], n)
        mask(u01[n], n)
    new, at = take(at)

    dummy = (u01[0] & 127,) * 2

    def steps(t, carry):
        old, now, new, at = carry

        @pl.loop(0, jnp.where(t == 1, 1, 0))
        def _(_):
            pass_on(5, 1, 2)
            pass_on(5, 0)
            pass_on(6, 0)
            pass_on(6, 1)

        new2, at = step(old, now, new, at, 0, 2)
        new3, at = step(now, new, new2, at, 2, 0)
        return new, new2, new3, at

    old, now, new, at = lax.fori_loop(0, 16, steps, (dummy, u01, new, at))
    step(old, now, new, at, 0, 2)
    step(now, new, None, None, 2, 0)
    for n in range(2):
        pv_stage(new[n], 2 + n)
    for n in range(2):
        fin(new[n])

    for d, dc in others:
        first(d, dc).wait_send()
        queries_to(d, dc).wait_send()
        frm = me.member(d, dc)
        outputs_to(frm.slot).wait_send()
        heads = pl.ds(pl.multiple_of(frm.head_block * 8, 8), 8)
        remote(ost.at[0], out_ref.at[:, heads, :], o_send.at[frm.slot], o_recv.at[frm.head_block], frm).wait_recv()
    for d in range(8):
        for half in range(2):
            forward(d, half).wait_send()
    for relayed in RELAYS:
        relay(*relayed).wait_send()


def shards(queries, keys, values):
    rows, heads, width = queries.shape
    start = lax.axis_index(("sx", "sy")) * rows
    positions = start + jnp.arange(rows, dtype=jnp.int32)
    angles = positions.astype(F32)[:, None] * frequencies(width)[None, :]
    cosine, sine = jnp.cos(angles), jnp.sin(angles)
    cos2 = jnp.concatenate([cosine, cosine], axis=1)
    sin2 = jnp.concatenate([-sine, sine], axis=1)
    def eightfold(a):
        return jnp.broadcast_to(a[:, None, :], (rows, 8, width)).reshape(rows * 8, width)

    dma = pltpu.SemaphoreType.DMA
    return pl.pallas_call(
        kernel,
        out_shape=jax.ShapeDtypeStruct((rows, heads, width), BF16),
        in_specs=[pl.BlockSpec(memory_space=pltpu.VMEM)] * 5,
        out_specs=pl.BlockSpec(memory_space=pltpu.VMEM),
        scratch_shapes=[
            pltpu.VMEM((2, 512, 128), F32),
            pltpu.VMEM((2, 8, 64, 128), BF16),
            pltpu.VMEM((16, 4, 128, 128), BF16),
            pltpu.VMEM((16, 4, 128, 128), BF16),
            pltpu.VMEM((2, 16, 4, 128, 128), BF16),
            pltpu.VMEM((16, 64, 8, 128), BF16),
            pltpu.VMEM((16, 2, KB, 128), BF16),
            pltpu.VMEM((16, 4, VR, 128), BF16),
            pltpu.VMEM((2, KB, 128), jnp.int32),
            *[pltpu.VMEM((KB, QW), F32)] * 4,
            *[pltpu.VMEM((8, KB, 128), BF16)] * 4,
            pltpu.VMEM((4, 1, QW), F32),
            pltpu.VMEM((4, 1, QW), F32),
            pltpu.VMEM((8, 1, QW), F32),
            pltpu.VMEM((8, VR, QW), F32),
            *[dma((16,))] * 10,
        ],
        compiler_params=pltpu.CompilerParams(
            collective_id=0, has_side_effects=True, vmem_limit_bytes=40 << 20
        ),
        name="fused",
    )(queries, keys, values, eightfold(cos2), eightfold(sin2))


def solution(mesh):
    placed = P(("sx", "sy"), None, None)
    return jax.shard_map(
        shards, mesh=mesh, in_specs=(placed, placed, placed), out_specs=placed, check_vma=False
    )
```

```python
import functools
import math

import jax
import jax.numpy as jnp
from jax import lax
from jax.experimental import pallas as pl
from jax.experimental.pallas import tpu as pltpu
from jax.sharding import PartitionSpec as P

MESH = pl.DeviceIdType.MESH
F32 = jnp.float32
BF16 = jnp.bfloat16
NEG = -1e30
CW = 256
QW = 1024
KB = 512
VR = 144
SCALE = math.log2(math.e) / math.sqrt(128.0)


def frequencies(head_width):
    half_index = jnp.arange(head_width // 2, dtype=F32)
    base_rate = jnp.power(F32(500000.0), -2.0 * half_index / head_width)
    wavelen = 2.0 * math.pi / base_rate
    smooth = (8192.0 / wavelen - 1.0) / 3.0
    blended = (1.0 - smooth) * base_rate / 8.0 + smooth * base_rate
    return jnp.where(
        wavelen < 2048.0, base_rate, jnp.where(wavelen > 8192.0, base_rate / 8.0, blended)
    )


def place(p, b):
    return p ^ (3 * b)


class Spot:
    def __init__(self, p, b, core):
        self.p, self.b, self.core = tuple(p), tuple(b), core

    @staticmethod
    def own():
        sx, sy = lax.axis_index("sx"), lax.axis_index("sy")
        xyz = (sx >> 2, (sy & 1) * 2 + ((sx >> 1) & 1), sy >> 1)
        return Spot([((c + 1) >> 1) & 1 for c in xyz], [c >> 1 for c in xyz], sx & 1)

    @property
    def sx(self):
        ylo = self.p[1] ^ self.b[1]
        return place(self.p[0], self.b[0]) * 4 + ylo * 2 + self.core

    @property
    def sy(self):
        return place(self.p[2], self.b[2]) * 2 + self.b[1]

    @property
    def device(self):
        return (self.sx, self.sy)

    @property
    def chip(self):
        return self.b[0] * 4 + self.b[1] * 2 + self.b[2]

    @property
    def head_block(self):
        return self.chip * 2 + self.core

    @property
    def pair_block(self):
        return (self.b[0] * 2 + self.b[1]) * 2 + self.core

    @property
    def slot(self):
        return self.pair_block * 2 + self.b[2]

    @property
    def part(self):
        return self.p[1] * 2 + self.p[2]

    def member(self, d, dc):
        return Spot(self.p, [b ^ ((d >> s) & 1) for b, s in zip(self.b, (2, 1, 0))], self.core ^ dc)

    def cousin(self, d):
        return Spot([p ^ ((d >> s) & 1) for p, s in zip(self.p, (2, 1, 0))], self.b, self.core)


ORDER = (7, 6, 1, 0, 4, 3, 5, 2)
HEAD_RUNS = 4
RELAYS = tuple((0, half, e) for e in (1, 2, 4) for half in range(2)) + (
    (2, 0, 1), (1, 1, 2), (1, 0, 4), (2, 1, 4), (4, 1, 1), (4, 0, 2), (3, 0, 4), (5, 1, 2))


def kernel(q_hbm, k_hbm, v_hbm, cos_ref, sin_ref, out_ref,
           q_ref, k_ref, v_ref, in_sem, flat_kv, kv_ref, qs, qr, kvb, ost, k2, vT, key_place, s0, s1, s2, s3, p0, p1, p2, p3, mx, al, m_ref, acc_ref,
           q_send, q_recv, k1_send, k1_recv, k2_send, k2_recv, f_send, f_recv, o_send, o_recv):
    S, W = (s0, s1, s2, s3), (p0, p1, p2, p3)
    H = CW // 128
    me = Spot.own()
    others = [(d, dc) for d in ORDER for dc in (1, 0) if (d, dc) != (0, 0)]

    def remote(src, dst, send, recv, spot):
        return pltpu.make_async_remote_copy(src_ref=src, dst_ref=dst, send_sem=send, recv_sem=recv, device_id=spot.device, device_id_type=MESH)

    inputs = [
        pltpu.make_async_copy(src, dst, in_sem.at[n])
        for n, (src, dst) in enumerate(((k_hbm, k_ref), (v_hbm, v_ref), (q_hbm, q_ref)))
    ]
    for copy in inputs:
        copy.start()
    barrier = pltpu.get_barrier_semaphore()
    for d, dc in others:
        pl.semaphore_signal(barrier, inc=1, device_id=me.member(d, dc).device, device_id_type=MESH)
    for d in range(1, 8):
        pl.semaphore_signal(barrier, inc=1, device_id=me.cousin(d).device, device_id_type=MESH)

    for copy in inputs:
        copy.wait()
    k = k_ref[...].astype(F32).reshape(512, 128)
    flat_kv[0] = k * cos_ref[...] + pltpu.roll(k, 64, 1) * sin_ref[...]
    flat_kv[1] = v_ref[...].astype(F32).reshape(512, 128)
    for role in range(2):
        for h in range(8):
            kv_ref[role, h] = flat_kv[role, pl.ds(h, 64, stride=8), :].astype(BF16)

    pl.semaphore_wait(barrier, len(others) + 7)

    def kv_spot(role, src):
        return kvb.at[role, src.sx, src.part, pl.ds(pl.multiple_of(src.b[2] * 64, 64), 64), :]

    def first(d, dc):
        to = me.member(d, dc)
        return remote(kv_ref.at[to.core, to.chip], kv_spot(to.core, me), k1_send.at[d * 2 + dc], k1_recv.at[me.slot], to)

    for d, dc in others:
        first(d, dc).start()
    kvb[me.core, me.sx, me.part, pl.ds(pl.multiple_of(me.b[2] * 64, 64), 64), :] = kv_ref[me.core, me.chip]

    def queries_to(d, dc):
        to = me.member(d, dc)
        return remote(qs.at[to.head_block], qr.at[me.slot], q_send.at[d * 2 + dc], q_recv.at[me.slot], to)

    for d in ORDER:
        to = me.member(d, 0)
        x = q_ref[:, pl.ds(pl.multiple_of(to.chip * 16, 16), 16), :].astype(F32)
        for c in range(2):
            part = x[:, c * 8:(c + 1) * 8, :].reshape(512, 128)
            turned = part * cos_ref[...] + pltpu.roll(part, 64, 1) * sin_ref[...]
            flat = turned.astype(BF16).T
            for h in range(4):
                qs[to.chip * 2 + c, h] = flat[:, h * 128:(h + 1) * 128]
        for dc in (1, 0):
            if (d, dc) != (0, 0):
                queries_to(d, dc).start()
    qr[me.slot] = qs[me.head_block]

    for d, dc in others:
        frm = me.member(d, dc)
        remote(kv_ref.at[0, 0], kv_spot(me.core, frm), k1_send.at[d * 2 + dc], k1_recv.at[frm.slot], frm).wait_recv()

    def region(spot, half):
        return kvb.at[me.core, pl.ds(pl.multiple_of(place(spot.p[0], half) * 4, 4), 4), spot.part]

    def relay(a, half, e):
        r = region(me.cousin(a), half)
        n = (a ^ e) * 2 + half
        return remote(r, r, k2_send.at[n], k2_recv.at[n], me.cousin(e))

    def forward(d, half):
        r = region(me.cousin(d), half)
        return remote(r, r, f_send.at[d * 2 + half], f_recv.at[d * 2 + half], me.member(0, 1))

    def arrived(d, half):
        r = region(me.cousin(d), half)
        return remote(r, r, k2_send.at[d * 2 + half], k2_recv.at[d * 2 + half], me.cousin(d))

    def handed(d, half):
        r = kvb.at[1 - me.core, pl.ds(pl.multiple_of(place(me.cousin(d).p[0], half) * 4, 4), 4), me.cousin(d).part]
        return remote(r, r, f_send.at[d * 2 + half], f_recv.at[d * 2 + half], me.member(0, 1))

    def pass_on(d, half, *axes):
        arrived(d, half).wait_recv()
        for e in axes:
            relay(d, half, e).start()
        forward(d, half).start()

    def ready(d):
        for half in range(2):
            handed(d, half).wait_recv()
        spot = me.cousin(d)
        h = spot.part

        @pl.loop(0, 2)
        def _(t):
            rows = pl.ds(pl.multiple_of(h * 128, 128), 128)
            for n in range(4):
                b = place(spot.p[0], t) * 4 + n
                vT[b, h, 0:128, :] = kvb[1, b, h].T
                wide = kvb[0, b, h].astype(F32) * SCALE
                hi = wide.astype(BF16)
                k2[b, 0, rows, :] = hi
                k2[b, 1, rows, :] = (wide - hi.astype(F32)).astype(BF16)

    for e, half in ((1, 1), (2, 0), (4, 1), (1, 0), (2, 1), (4, 0)):
        relay(0, half, e).start()
    for half in range(2):
        forward(0, half).start()

    row = lax.broadcasted_iota(jnp.int32, (KB, 128), 0)
    for ylo in range(2):
        z_at = ((row >> 7) & 1) ^ (3 * ((row >> 6) & 1))
        key_place[ylo] = (z_at * 2 + ((row >> 8) ^ ylo)) * 64 + (row & 63)

    acc_ref[...] = jnp.zeros_like(acc_ref)
    al[...] = jnp.zeros_like(al)
    for w in W[2:]:
        w[...] = jnp.zeros_like(w)

    @pl.loop(0, 16)
    def _(b):
        for h in range(4):
            vT[b, h, 128:VR, :] = jnp.ones((VR - 128, 128), BF16)

    ready(0)
    pass_on(2, 0, 1)
    pass_on(1, 1, 2)
    pass_on(1, 0, 4)
    pass_on(2, 1, 4)
    pass_on(4, 1, 1)
    pass_on(4, 0, 2)
    ready(1)
    ready(2)
    pass_on(3, 0, 4)
    pass_on(3, 1)
    ready(3)

    px = me.p[0]


    own_block = me.pair_block

    def early_block(k):
        g = k >> 1
        return own_block ^ ((1 - (g & 1)) * 4 + (1 - (g >> 1)) * 2 + (k & 1))

    def source(i, bz):
        return Spot(me.p, (i >> 2, (i >> 1) & 1, bz), i & 1)

    def rank(i):
        return (i & 4) + ((me.p[1] ^ ((i >> 1) & 1)) * 2) + (i & 1)

    def run(n):
        k = jnp.where(n < HEAD_RUNS, n, jnp.where(n < 2 * HEAD_RUNS, n - HEAD_RUNS, n >> 1))
        side = jnp.where(n < HEAD_RUNS, 0, jnp.where(n < 2 * HEAD_RUNS, 1, n & 1))
        return early_block(k), side

    def length(n):
        i, side = run(n)
        return jnp.where(side == 0, rank(i) + 1, jnp.where(px == 0, (i & 4) * 2, 4))

    def unit(at):
        n, r, seen = at
        i, side = run(n)
        mine = (px ^ (3 * (r >> 2))) * 4 + (r & 3)
        other = r + 4 * (1 - px)
        end = jnp.where(r + 1 == length(n), 1, 0)
        far = jnp.where(side == 1, 1, 0)
        done = end * jnp.where(far + (1 - (px | (i >> 2))) > 0, 1, 0)
        first_of = jnp.where(r == 0, 1, 0) * (1 - far)
        code = i + 8 * jnp.where(side == 0, mine, other) + 128 * first_of + 256 * done + 512 * end * (1 - far) + 1024 * far * (1 - seen)
        n1 = n + 1
        n1 = jnp.where(length(n1) == 0, n1 + 1, n1)
        n1 = jnp.where(length(n1) == 0, n1 + 1, n1)
        after = jnp.where(end == 1, jnp.minimum(n1, 15), n), jnp.where(end == 1, 0, r + 1), seen | far
        return code, after

    def qblock(u):
        return u & 7

    def kblock(u):
        return (u >> 3) & 15

    def queries_in(u):
        @pl.loop(0, (u >> 7) & 1)
        def _(_):
            i = qblock(u)
            for bz in range(2):
                s = 2 * i + bz

                @pl.when(s != me.slot)
                def _():
                    remote(qs.at[0], qr.at[s], q_send.at[0], q_recv.at[s], me.member(1, 0)).wait_recv()

    def qk_stage(u, slot, pieces=range(QW // CW)):
        i, b = qblock(u), kblock(u)
        for n in pieces:
            cols = pl.ds(n * CW, CW)
            kk = jnp.concatenate([k2[b, 0], k2[b, 1]], axis=1)
            qq = jnp.concatenate([qr[2 * i + (n * H + h) // 4, (n * H + h) % 4] for h in range(H)], axis=1)
            qq = jnp.concatenate([qq, qq], axis=0)
            s = jnp.dot(kk, qq, preferred_element_type=F32)
            S[slot][:, cols] = s
            mx[slot, :, cols] = jnp.max(s, axis=0, keepdims=True)

    def mask(u, slot):
        @pl.loop(0, (u >> 9) & 1)
        def _(_):
            here = source(qblock(u), 0)
            key_at = key_place[me.p[1] ^ here.b[1]]
            lane = lax.broadcasted_iota(jnp.int32, (1, 128), 1) >> 3
            for n in range(QW // 128):
                cols = pl.ds(n * 128, 128)
                query_at = lane + (source(qblock(u), n // 4).sy * 64 + n % 4 * 16)
                s = jnp.where(key_at <= query_at, S[slot][:, cols], NEG)
                S[slot][:, cols] = s
                mx[slot, :, cols] = jnp.max(s, axis=0, keepdims=True)

    def soft_stage(u, slot, pieces=range(QW // CW)):
        i = qblock(u)
        for n in pieces:
            cols = pl.ds(n * CW, CW)
            m_old = jnp.where((u >> 7) & 1 == 1, NEG, m_ref[i, :, cols])
            m_new = jnp.maximum(m_old, mx[slot, :, cols])
            m_ref[i, :, cols] = m_new
            al[slot, :, cols] = jnp.exp2(m_old - m_new)
            w = jnp.exp2(S[slot][:, cols] - m_new).astype(BF16)
            for h in range(H):
                W[slot][n * H + h] = w[:, h * 128:(h + 1) * 128]

    def pv_stage(u, slot):
        i, b = qblock(u), kblock(u)
        for n in range(QW // CW):
            cols = pl.ds(n * CW, CW)
            ww = jnp.concatenate([W[slot][n * H + h] for h in range(H)], axis=1)
            vv = jnp.concatenate([vT[b, h] for h in range(4)], axis=1)
            acc_ref[i, :, cols] = acc_ref[i, :, cols] * al[slot, :, cols] + jnp.dot(vv, ww, preferred_element_type=F32)

    def outputs_to(s):
        to = Spot(me.p, (s >> 3, (s >> 2) & 1, s & 1), (s >> 1) & 1)
        heads = pl.ds(pl.multiple_of(me.head_block * 8, 8), 8)
        return remote(ost.at[s], out_ref.at[:, heads, :], o_send.at[s], o_recv.at[me.head_block], to)

    def fin(u):
        @pl.loop(0, (u >> 8) & 1)
        def _(_):
            i = qblock(u)
            o = acc_ref[i, 0:128, :] * (1.0 / acc_ref[i, 128:129, :])
            for bz in range(2):
                for t in range(2):
                    c0 = bz * 512 + t * 256
                    ost[2 * i + bz, pl.ds(t * 32, 32)] = o[:, c0:c0 + 256].T.reshape(32, 8, 128).astype(BF16)
            for bz in range(2):
                s = 2 * i + bz

                @pl.when(s != me.slot)
                def _():
                    outputs_to(s).start()

                @pl.when(s == me.slot)
                def _():
                    out_ref[:, pl.ds(pl.multiple_of(me.head_block * 8, 8), 8), :] = ost[s]

    def other_keys(u):
        @pl.loop(0, (u >> 10) & 1)
        def _(_):
            pass_on(7, 0)
            pass_on(7, 1)
            for d in range(4, 8):
                ready(d)

    def any_of(bits, units):
        got = units[0] | units[1]
        return jnp.where((got & bits) != 0, 1, 0)

    def step(old, now, new, at, cur, nxt):
        if new is None:
            for n in range(2):
                soft_stage(now[n], cur + n)
            for n in range(2):
                pv_stage(old[n], nxt + n)
            for n in range(2):
                fin(old[n])
            return None

        @pl.loop(0, any_of(128 + 1024, new))
        def _(_):
            for n in range(2):
                queries_in(new[n])
                other_keys(new[n])

        ahead, at = take(at)
        for n in range(2):
            for piece in range(QW // CW):
                qk_stage(new[n], nxt + n, (piece,))
                soft_stage(now[n], cur + n, (piece,))
        for n in range(2):
            pv_stage(old[n], nxt + n)

        @pl.loop(0, jnp.maximum(any_of(512, new), any_of(256, old)))
        def _(_):
            for n in range(2):
                mask(new[n], nxt + n)
            for n in range(2):
                fin(old[n])

        return ahead, at

    def take(at):
        u, at = unit(at)
        v, at = unit(at)
        return (u, v), at

    z = jnp.int32(0)
    u01, at = take((z, z, z))
    for n in range(2):
        queries_in(u01[n])
        qk_stage(u01[n], n)
        mask(u01[n], n)
    new, at = take(at)

    dummy = (u01[0] & 127,) * 2

    def steps(t, carry):
        old, now, new, at = carry

        @pl.loop(0, jnp.where(t == 1, 1, 0))
        def _(_):
            pass_on(5, 1, 2)
            pass_on(5, 0)
            pass_on(6, 0)
            pass_on(6, 1)

        new2, at = step(old, now, new, at, 0, 2)
        new3, at = step(now, new, new2, at, 2, 0)
        return new, new2, new3, at

    old, now, new, at = lax.fori_loop(0, 16, steps, (dummy, u01, new, at))
    step(old, now, new, at, 0, 2)
    step(now, new, None, None, 2, 0)
    for n in range(2):
        pv_stage(new[n], 2 + n)
    for n in range(2):
        fin(new[n])

    for d, dc in others:
        first(d, dc).wait_send()
        queries_to(d, dc).wait_send()
        frm = me.member(d, dc)
        outputs_to(frm.slot).wait_send()
        heads = pl.ds(pl.multiple_of(frm.head_block * 8, 8), 8)
        remote(ost.at[0], out_ref.at[:, heads, :], o_send.at[frm.slot], o_recv.at[frm.head_block], frm).wait_recv()
    for d in range(8):
        for half in range(2):
            forward(d, half).wait_send()
    for relayed in RELAYS:
        relay(*relayed).wait_send()


def shards(queries, keys, values):
    rows, heads, width = queries.shape
    start = lax.axis_index(("sx", "sy")) * rows
    positions = start + jnp.arange(rows, dtype=jnp.int32)
    angles = positions.astype(F32)[:, None] * frequencies(width)[None, :]
    cosine, sine = jnp.cos(angles), jnp.sin(angles)
    cos2 = jnp.concatenate([cosine, cosine], axis=1)
    sin2 = jnp.concatenate([-sine, sine], axis=1)
    def eightfold(a):
        return jnp.broadcast_to(a[:, None, :], (rows, 8, width)).reshape(rows * 8, width)

    dma = pltpu.SemaphoreType.DMA
    return pl.pallas_call(
        kernel,
        out_shape=jax.ShapeDtypeStruct((rows, heads, width), BF16),
        in_specs=[pl.BlockSpec(memory_space=pltpu.HBM)] * 3 + [pl.BlockSpec(memory_space=pltpu.VMEM)] * 2,
        out_specs=pl.BlockSpec(memory_space=pltpu.VMEM),
        scratch_shapes=[
            pltpu.VMEM((rows, heads, width), BF16),
            pltpu.VMEM((rows, 8, width), BF16),
            pltpu.VMEM((rows, 8, width), BF16),
            dma((3,)),
            pltpu.VMEM((2, 512, 128), F32),
            pltpu.VMEM((2, 8, 64, 128), BF16),
            pltpu.VMEM((16, 4, 128, 128), BF16),
            pltpu.VMEM((16, 4, 128, 128), BF16),
            pltpu.VMEM((2, 16, 4, 128, 128), BF16),
            pltpu.VMEM((16, 64, 8, 128), BF16),
            pltpu.VMEM((16, 2, KB, 128), BF16),
            pltpu.VMEM((16, 4, VR, 128), BF16),
            pltpu.VMEM((2, KB, 128), jnp.int32),
            *[pltpu.VMEM((KB, QW), F32)] * 4,
            *[pltpu.VMEM((8, KB, 128), BF16)] * 4,
            pltpu.VMEM((4, 1, QW), F32),
            pltpu.VMEM((4, 1, QW), F32),
            pltpu.VMEM((8, 1, QW), F32),
            pltpu.VMEM((8, VR, QW), F32),
            *[dma((16,))] * 10,
        ],
        compiler_params=pltpu.CompilerParams(
            collective_id=0, has_side_effects=True, vmem_limit_bytes=40 << 20
        ),
        name="fused",
    )(
        *(pltpu.with_memory_space_constraint(a, pltpu.HBM) for a in (queries, keys, values)),
        eightfold(cos2),
        eightfold(sin2),
    )


def solution(mesh):
    placed = P(("sx", "sy"), None, None)
    return jax.shard_map(
        shards, mesh=mesh, in_specs=(placed, placed, placed), out_specs=placed, check_vma=False
    )
```

```python
import functools
import math

import jax
import jax.numpy as jnp
from jax import lax
from jax.experimental import pallas as pl
from jax.experimental.pallas import tpu as pltpu
from jax.sharding import PartitionSpec as P

MESH = pl.DeviceIdType.MESH
F32 = jnp.float32
BF16 = jnp.bfloat16
NEG = -1e30
CW = 256
QW = 1024
KB = 512
VR = 144
SCALE = math.log2(math.e) / math.sqrt(128.0)


def frequencies(head_width):
    half_index = jnp.arange(head_width // 2, dtype=F32)
    base_rate = jnp.power(F32(500000.0), -2.0 * half_index / head_width)
    wavelen = 2.0 * math.pi / base_rate
    smooth = (8192.0 / wavelen - 1.0) / 3.0
    blended = (1.0 - smooth) * base_rate / 8.0 + smooth * base_rate
    return jnp.where(
        wavelen < 2048.0, base_rate, jnp.where(wavelen > 8192.0, base_rate / 8.0, blended)
    )


def place(p, b):
    return p ^ (3 * b)


class Spot:
    def __init__(self, p, b, core):
        self.p, self.b, self.core = tuple(p), tuple(b), core

    @staticmethod
    def own():
        sx, sy = lax.axis_index("sx"), lax.axis_index("sy")
        xyz = (sx >> 2, (sy & 1) * 2 + ((sx >> 1) & 1), sy >> 1)
        return Spot([((c + 1) >> 1) & 1 for c in xyz], [c >> 1 for c in xyz], sx & 1)

    @property
    def sx(self):
        ylo = self.p[1] ^ self.b[1]
        return place(self.p[0], self.b[0]) * 4 + ylo * 2 + self.core

    @property
    def sy(self):
        return place(self.p[2], self.b[2]) * 2 + self.b[1]

    @property
    def device(self):
        return (self.sx, self.sy)

    @property
    def chip(self):
        return self.b[0] * 4 + self.b[1] * 2 + self.b[2]

    @property
    def head_block(self):
        return self.chip * 2 + self.core

    @property
    def pair_block(self):
        return (self.b[0] * 2 + self.b[1]) * 2 + self.core

    @property
    def slot(self):
        return self.pair_block * 2 + self.b[2]

    @property
    def part(self):
        return self.p[1] * 2 + self.p[2]

    def member(self, d, dc):
        return Spot(self.p, [b ^ ((d >> s) & 1) for b, s in zip(self.b, (2, 1, 0))], self.core ^ dc)

    def cousin(self, d):
        return Spot([p ^ ((d >> s) & 1) for p, s in zip(self.p, (2, 1, 0))], self.b, self.core)


ORDER = (7, 6, 1, 0, 4, 3, 5, 2)
AHEAD = 4
HEAD_RUNS = 4
RELAYS = tuple((0, half, e) for e in (1, 2, 4) for half in range(2)) + (
    (2, 0, 1), (1, 1, 2), (1, 0, 4), (2, 1, 4), (4, 1, 1), (4, 0, 2), (3, 0, 4), (5, 1, 2))


def kernel(q_hbm, k_hbm, v_hbm, cos_ref, sin_ref, out_ref,
           q_ref, k_ref, v_ref, in_sem, flat_kv, kv_ref, qs, qr, kvb, ost, k2, vT, key_place, s0, s1, s2, s3, p0, p1, p2, p3, mx, al, m_ref, acc_ref,
           q_send, q_recv, k1_send, k1_recv, k2_send, k2_recv, f_send, f_recv, o_send, o_recv):
    S, W = (s0, s1, s2, s3), (p0, p1, p2, p3)
    H = CW // 128
    me = Spot.own()
    others = [(d, dc) for d in ORDER for dc in (1, 0) if (d, dc) != (0, 0)]

    def remote(src, dst, send, recv, spot):
        return pltpu.make_async_remote_copy(src_ref=src, dst_ref=dst, send_sem=send, recv_sem=recv, device_id=spot.device, device_id_type=MESH)

    inputs = [
        pltpu.make_async_copy(src, dst, in_sem.at[n])
        for n, (src, dst) in enumerate(((k_hbm, k_ref), (v_hbm, v_ref), (q_hbm, q_ref)))
    ]
    for copy in inputs:
        copy.start()
    barrier = pltpu.get_barrier_semaphore()
    for d, dc in others:
        pl.semaphore_signal(barrier, inc=1, device_id=me.member(d, dc).device, device_id_type=MESH)
    for d in range(1, 8):
        pl.semaphore_signal(barrier, inc=1, device_id=me.cousin(d).device, device_id_type=MESH)

    row = lax.broadcasted_iota(jnp.int32, (KB, 128), 0)
    for ylo in range(2):
        z_at = ((row >> 7) & 1) ^ (3 * ((row >> 6) & 1))
        key_place[ylo] = (z_at * 2 + ((row >> 8) ^ ylo)) * 64 + (row & 63)

    acc_ref[...] = jnp.zeros_like(acc_ref)
    al[...] = jnp.zeros_like(al)
    for w in W[2:]:
        w[...] = jnp.zeros_like(w)

    @pl.loop(0, 16)
    def _(b):
        for h in range(4):
            vT[b, h, 128:VR, :] = jnp.ones((VR - 128, 128), BF16)

    for copy in inputs:
        copy.wait()
    k = k_ref[...].astype(F32).reshape(512, 128)
    flat_kv[0] = k * cos_ref[...] + pltpu.roll(k, 64, 1) * sin_ref[...]
    flat_kv[1] = v_ref[...].astype(F32).reshape(512, 128)
    for role in range(2):
        for h in range(8):
            kv_ref[role, h] = flat_kv[role, pl.ds(h, 64, stride=8), :].astype(BF16)

    def rotate_for(d):
        to = me.member(d, 0)
        x = q_ref[:, pl.ds(pl.multiple_of(to.chip * 16, 16), 16), :].astype(F32)
        for c in range(2):
            part = x[:, c * 8:(c + 1) * 8, :].reshape(512, 128)
            turned = part * cos_ref[...] + pltpu.roll(part, 64, 1) * sin_ref[...]
            flat = turned.astype(BF16).T
            for h in range(4):
                qs[to.chip * 2 + c, h] = flat[:, h * 128:(h + 1) * 128]

    for d in ORDER[:AHEAD]:
        rotate_for(d)
    pl.semaphore_wait(barrier, len(others) + 7)

    def kv_spot(role, src):
        return kvb.at[role, src.sx, src.part, pl.ds(pl.multiple_of(src.b[2] * 64, 64), 64), :]

    def first(d, dc):
        to = me.member(d, dc)
        return remote(kv_ref.at[to.core, to.chip], kv_spot(to.core, me), k1_send.at[d * 2 + dc], k1_recv.at[me.slot], to)

    for d, dc in others:
        first(d, dc).start()
    kvb[me.core, me.sx, me.part, pl.ds(pl.multiple_of(me.b[2] * 64, 64), 64), :] = kv_ref[me.core, me.chip]

    def queries_to(d, dc):
        to = me.member(d, dc)
        return remote(qs.at[to.head_block], qr.at[me.slot], q_send.at[d * 2 + dc], q_recv.at[me.slot], to)

    for n, d in enumerate(ORDER):
        if n >= AHEAD:
            rotate_for(d)
        for dc in (1, 0):
            if (d, dc) != (0, 0):
                queries_to(d, dc).start()
    qr[me.slot] = qs[me.head_block]

    for d, dc in others:
        frm = me.member(d, dc)
        remote(kv_ref.at[0, 0], kv_spot(me.core, frm), k1_send.at[d * 2 + dc], k1_recv.at[frm.slot], frm).wait_recv()

    def region(spot, half):
        return kvb.at[me.core, pl.ds(pl.multiple_of(place(spot.p[0], half) * 4, 4), 4), spot.part]

    def relay(a, half, e):
        r = region(me.cousin(a), half)
        n = (a ^ e) * 2 + half
        return remote(r, r, k2_send.at[n], k2_recv.at[n], me.cousin(e))

    def forward(d, half):
        r = region(me.cousin(d), half)
        return remote(r, r, f_send.at[d * 2 + half], f_recv.at[d * 2 + half], me.member(0, 1))

    def arrived(d, half):
        r = region(me.cousin(d), half)
        return remote(r, r, k2_send.at[d * 2 + half], k2_recv.at[d * 2 + half], me.cousin(d))

    def handed(d, half):
        r = kvb.at[1 - me.core, pl.ds(pl.multiple_of(place(me.cousin(d).p[0], half) * 4, 4), 4), me.cousin(d).part]
        return remote(r, r, f_send.at[d * 2 + half], f_recv.at[d * 2 + half], me.member(0, 1))

    def pass_on(d, half, *axes):
        arrived(d, half).wait_recv()
        for e in axes:
            relay(d, half, e).start()
        forward(d, half).start()

    def ready(d):
        for half in range(2):
            handed(d, half).wait_recv()
        spot = me.cousin(d)
        h = spot.part

        @pl.loop(0, 2)
        def _(t):
            rows = pl.ds(pl.multiple_of(h * 128, 128), 128)
            for n in range(4):
                b = place(spot.p[0], t) * 4 + n
                vT[b, h, 0:128, :] = kvb[1, b, h].T
                wide = kvb[0, b, h].astype(F32) * SCALE
                hi = wide.astype(BF16)
                k2[b, 0, rows, :] = hi
                k2[b, 1, rows, :] = (wide - hi.astype(F32)).astype(BF16)

    for e, half in ((1, 1), (2, 0), (4, 1), (1, 0), (2, 1), (4, 0)):
        relay(0, half, e).start()
    for half in range(2):
        forward(0, half).start()

    ready(0)
    pass_on(2, 0, 1)
    pass_on(1, 1, 2)
    pass_on(1, 0, 4)
    pass_on(2, 1, 4)
    pass_on(4, 1, 1)
    pass_on(4, 0, 2)
    ready(1)
    ready(2)
    pass_on(3, 0, 4)
    pass_on(3, 1)
    ready(3)

    px = me.p[0]


    own_block = me.pair_block

    def early_block(k):
        g = k >> 1
        return own_block ^ ((1 - (g & 1)) * 4 + (1 - (g >> 1)) * 2 + (k & 1))

    def source(i, bz):
        return Spot(me.p, (i >> 2, (i >> 1) & 1, bz), i & 1)

    def rank(i):
        return (i & 4) + ((me.p[1] ^ ((i >> 1) & 1)) * 2) + (i & 1)

    def run(n):
        k = jnp.where(n < HEAD_RUNS, n, jnp.where(n < 2 * HEAD_RUNS, n - HEAD_RUNS, n >> 1))
        side = jnp.where(n < HEAD_RUNS, 0, jnp.where(n < 2 * HEAD_RUNS, 1, n & 1))
        return early_block(k), side

    def length(n):
        i, side = run(n)
        return jnp.where(side == 0, rank(i) + 1, jnp.where(px == 0, (i & 4) * 2, 4))

    def unit(at):
        n, r, seen = at
        i, side = run(n)
        mine = (px ^ (3 * (r >> 2))) * 4 + (r & 3)
        other = r + 4 * (1 - px)
        end = jnp.where(r + 1 == length(n), 1, 0)
        far = jnp.where(side == 1, 1, 0)
        done = end * jnp.where(far + (1 - (px | (i >> 2))) > 0, 1, 0)
        first_of = jnp.where(r == 0, 1, 0) * (1 - far)
        code = i + 8 * jnp.where(side == 0, mine, other) + 128 * first_of + 256 * done + 512 * end * (1 - far) + 1024 * far * (1 - seen)
        n1 = n + 1
        n1 = jnp.where(length(n1) == 0, n1 + 1, n1)
        n1 = jnp.where(length(n1) == 0, n1 + 1, n1)
        after = jnp.where(end == 1, jnp.minimum(n1, 15), n), jnp.where(end == 1, 0, r + 1), seen | far
        return code, after

    def qblock(u):
        return u & 7

    def kblock(u):
        return (u >> 3) & 15

    def queries_in(u):
        @pl.loop(0, (u >> 7) & 1)
        def _(_):
            i = qblock(u)
            for bz in range(2):
                s = 2 * i + bz

                @pl.when(s != me.slot)
                def _():
                    remote(qs.at[0], qr.at[s], q_send.at[0], q_recv.at[s], me.member(1, 0)).wait_recv()

    def qk_stage(u, slot, pieces=range(QW // CW)):
        i, b = qblock(u), kblock(u)
        for n in pieces:
            cols = pl.ds(n * CW, CW)
            kk = jnp.concatenate([k2[b, 0], k2[b, 1]], axis=1)
            qq = jnp.concatenate([qr[2 * i + (n * H + h) // 4, (n * H + h) % 4] for h in range(H)], axis=1)
            qq = jnp.concatenate([qq, qq], axis=0)
            s = jnp.dot(kk, qq, preferred_element_type=F32)
            S[slot][:, cols] = s
            mx[slot, :, cols] = jnp.max(s, axis=0, keepdims=True)

    def mask(u, slot):
        @pl.loop(0, (u >> 9) & 1)
        def _(_):
            here = source(qblock(u), 0)
            key_at = key_place[me.p[1] ^ here.b[1]]
            lane = lax.broadcasted_iota(jnp.int32, (1, 128), 1) >> 3
            for n in range(QW // 128):
                cols = pl.ds(n * 128, 128)
                query_at = lane + (source(qblock(u), n // 4).sy * 64 + n % 4 * 16)
                s = jnp.where(key_at <= query_at, S[slot][:, cols], NEG)
                S[slot][:, cols] = s
                mx[slot, :, cols] = jnp.max(s, axis=0, keepdims=True)

    def soft_stage(u, slot, pieces=range(QW // CW)):
        i = qblock(u)
        for n in pieces:
            cols = pl.ds(n * CW, CW)
            m_old = jnp.where((u >> 7) & 1 == 1, NEG, m_ref[i, :, cols])
            m_new = jnp.maximum(m_old, mx[slot, :, cols])
            m_ref[i, :, cols] = m_new
            al[slot, :, cols] = jnp.exp2(m_old - m_new)
            w = jnp.exp2(S[slot][:, cols] - m_new).astype(BF16)
            for h in range(H):
                W[slot][n * H + h] = w[:, h * 128:(h + 1) * 128]

    def pv_stage(u, slot):
        i, b = qblock(u), kblock(u)
        for n in range(QW // CW):
            cols = pl.ds(n * CW, CW)
            ww = jnp.concatenate([W[slot][n * H + h] for h in range(H)], axis=1)
            vv = jnp.concatenate([vT[b, h] for h in range(4)], axis=1)
            acc_ref[i, :, cols] = acc_ref[i, :, cols] * al[slot, :, cols] + jnp.dot(vv, ww, preferred_element_type=F32)

    def outputs_to(s):
        to = Spot(me.p, (s >> 3, (s >> 2) & 1, s & 1), (s >> 1) & 1)
        heads = pl.ds(pl.multiple_of(me.head_block * 8, 8), 8)
        return remote(ost.at[s], out_ref.at[:, heads, :], o_send.at[s], o_recv.at[me.head_block], to)

    def fin(u):
        @pl.loop(0, (u >> 8) & 1)
        def _(_):
            i = qblock(u)
            o = acc_ref[i, 0:128, :] * (1.0 / acc_ref[i, 128:129, :])
            for bz in range(2):
                for t in range(2):
                    c0 = bz * 512 + t * 256
                    ost[2 * i + bz, pl.ds(t * 32, 32)] = o[:, c0:c0 + 256].T.reshape(32, 8, 128).astype(BF16)
            for bz in range(2):
                s = 2 * i + bz

                @pl.when(s != me.slot)
                def _():
                    outputs_to(s).start()

                @pl.when(s == me.slot)
                def _():
                    out_ref[:, pl.ds(pl.multiple_of(me.head_block * 8, 8), 8), :] = ost[s]

    def other_keys(u):
        @pl.loop(0, (u >> 10) & 1)
        def _(_):
            pass_on(7, 0)
            pass_on(7, 1)
            for d in range(4, 8):
                ready(d)

    def any_of(bits, units):
        got = units[0] | units[1]
        return jnp.where((got & bits) != 0, 1, 0)

    def step(old, now, new, at, cur, nxt):
        if new is None:
            for n in range(2):
                soft_stage(now[n], cur + n)
            for n in range(2):
                pv_stage(old[n], nxt + n)
            for n in range(2):
                fin(old[n])
            return None

        @pl.loop(0, any_of(128 + 1024, new))
        def _(_):
            for n in range(2):
                queries_in(new[n])
                other_keys(new[n])

        ahead, at = take(at)
        for n in range(2):
            for piece in range(QW // CW):
                qk_stage(new[n], nxt + n, (piece,))
                soft_stage(now[n], cur + n, (piece,))
        for n in range(2):
            pv_stage(old[n], nxt + n)

        @pl.loop(0, jnp.maximum(any_of(512, new), any_of(256, old)))
        def _(_):
            for n in range(2):
                mask(new[n], nxt + n)
            for n in range(2):
                fin(old[n])

        return ahead, at

    def take(at):
        u, at = unit(at)
        v, at = unit(at)
        return (u, v), at

    z = jnp.int32(0)
    u01, at = take((z, z, z))
    for n in range(2):
        queries_in(u01[n])
        qk_stage(u01[n], n)
        mask(u01[n], n)
    new, at = take(at)

    dummy = (u01[0] & 127,) * 2

    def steps(t, carry):
        old, now, new, at = carry

        @pl.loop(0, jnp.where(t == 2, 1, 0))
        def _(_):
            pass_on(5, 1, 2)
            pass_on(5, 0)
            pass_on(6, 0)
            pass_on(6, 1)

        new2, at = step(old, now, new, at, 0, 2)
        new3, at = step(now, new, new2, at, 2, 0)
        return new, new2, new3, at

    old, now, new, at = lax.fori_loop(0, 16, steps, (dummy, u01, new, at))
    step(old, now, new, at, 0, 2)
    step(now, new, None, None, 2, 0)
    for n in range(2):
        pv_stage(new[n], 2 + n)
    for n in range(2):
        fin(new[n])

    for d, dc in others:
        first(d, dc).wait_send()
        queries_to(d, dc).wait_send()
        frm = me.member(d, dc)
        outputs_to(frm.slot).wait_send()
        heads = pl.ds(pl.multiple_of(frm.head_block * 8, 8), 8)
        remote(ost.at[0], out_ref.at[:, heads, :], o_send.at[frm.slot], o_recv.at[frm.head_block], frm).wait_recv()
    for d in range(8):
        for half in range(2):
            forward(d, half).wait_send()
    for relayed in RELAYS:
        relay(*relayed).wait_send()


def shards(queries, keys, values):
    rows, heads, width = queries.shape
    start = lax.axis_index(("sx", "sy")) * rows
    positions = start + jnp.arange(rows, dtype=jnp.int32)
    angles = positions.astype(F32)[:, None] * frequencies(width)[None, :]
    cosine, sine = jnp.cos(angles), jnp.sin(angles)
    cos2 = jnp.concatenate([cosine, cosine], axis=1)
    sin2 = jnp.concatenate([-sine, sine], axis=1)
    def eightfold(a):
        return jnp.broadcast_to(a[:, None, :], (rows, 8, width)).reshape(rows * 8, width)

    dma = pltpu.SemaphoreType.DMA
    return pl.pallas_call(
        kernel,
        out_shape=jax.ShapeDtypeStruct((rows, heads, width), BF16),
        in_specs=[pl.BlockSpec(memory_space=pltpu.HBM)] * 3 + [pl.BlockSpec(memory_space=pltpu.VMEM)] * 2,
        out_specs=pl.BlockSpec(memory_space=pltpu.VMEM),
        scratch_shapes=[
            pltpu.VMEM((rows, heads, width), BF16),
            pltpu.VMEM((rows, 8, width), BF16),
            pltpu.VMEM((rows, 8, width), BF16),
            dma((3,)),
            pltpu.VMEM((2, 512, 128), F32),
            pltpu.VMEM((2, 8, 64, 128), BF16),
            pltpu.VMEM((16, 4, 128, 128), BF16),
            pltpu.VMEM((16, 4, 128, 128), BF16),
            pltpu.VMEM((2, 16, 4, 128, 128), BF16),
            pltpu.VMEM((16, 64, 8, 128), BF16),
            pltpu.VMEM((16, 2, KB, 128), BF16),
            pltpu.VMEM((16, 4, VR, 128), BF16),
            pltpu.VMEM((2, KB, 128), jnp.int32),
            *[pltpu.VMEM((KB, QW), F32)] * 4,
            *[pltpu.VMEM((8, KB, 128), BF16)] * 4,
            pltpu.VMEM((4, 1, QW), F32),
            pltpu.VMEM((4, 1, QW), F32),
            pltpu.VMEM((8, 1, QW), F32),
            pltpu.VMEM((8, VR, QW), F32),
            *[dma((16,))] * 10,
        ],
        compiler_params=pltpu.CompilerParams(
            collective_id=0, has_side_effects=True, vmem_limit_bytes=40 << 20
        ),
        name="fused",
    )(
        *(pltpu.with_memory_space_constraint(a, pltpu.HBM) for a in (queries, keys, values)),
        eightfold(cos2),
        eightfold(sin2),
    )


def solution(mesh):
    placed = P(("sx", "sy"), None, None)
    return jax.shard_map(
        shards, mesh=mesh, in_specs=(placed, placed, placed), out_specs=placed, check_vma=False
    )
```

```python
import functools
import math

import jax
import jax.numpy as jnp
from jax import lax
from jax.experimental import pallas as pl
from jax.experimental.pallas import tpu as pltpu
from jax.sharding import PartitionSpec as P

MESH = pl.DeviceIdType.MESH
F32 = jnp.float32
BF16 = jnp.bfloat16
NEG = -1e30
CW = 256
QW = 1024
KB = 512
VR = 144
SCALE = math.log2(math.e) / math.sqrt(128.0)


def frequencies(head_width):
    half_index = jnp.arange(head_width // 2, dtype=F32)
    base_rate = jnp.power(F32(500000.0), -2.0 * half_index / head_width)
    wavelen = 2.0 * math.pi / base_rate
    smooth = (8192.0 / wavelen - 1.0) / 3.0
    blended = (1.0 - smooth) * base_rate / 8.0 + smooth * base_rate
    return jnp.where(
        wavelen < 2048.0, base_rate, jnp.where(wavelen > 8192.0, base_rate / 8.0, blended)
    )


def place(p, b):
    return p ^ (3 * b)


class Spot:
    def __init__(self, p, b, core):
        self.p, self.b, self.core = tuple(p), tuple(b), core

    @staticmethod
    def own():
        sx, sy = lax.axis_index("sx"), lax.axis_index("sy")
        xyz = (sx >> 2, (sy & 1) * 2 + ((sx >> 1) & 1), sy >> 1)
        return Spot([((c + 1) >> 1) & 1 for c in xyz], [c >> 1 for c in xyz], sx & 1)

    @property
    def sx(self):
        ylo = self.p[1] ^ self.b[1]
        return place(self.p[0], self.b[0]) * 4 + ylo * 2 + self.core

    @property
    def sy(self):
        return place(self.p[2], self.b[2]) * 2 + self.b[1]

    @property
    def device(self):
        return (self.sx, self.sy)

    @property
    def chip(self):
        return self.b[0] * 4 + self.b[1] * 2 + self.b[2]

    @property
    def head_block(self):
        return self.chip * 2 + self.core

    @property
    def pair_block(self):
        return (self.b[0] * 2 + self.b[1]) * 2 + self.core

    @property
    def slot(self):
        return self.pair_block * 2 + self.b[2]

    @property
    def part(self):
        return self.p[1] * 2 + self.p[2]

    def member(self, d, dc):
        return Spot(self.p, [b ^ ((d >> s) & 1) for b, s in zip(self.b, (2, 1, 0))], self.core ^ dc)

    def cousin(self, d):
        return Spot([p ^ ((d >> s) & 1) for p, s in zip(self.p, (2, 1, 0))], self.b, self.core)


ORDER = (7, 6, 1, 0, 4, 3, 5, 2)
AHEAD = 4
HEAD_RUNS = 4
RELAYS = tuple((0, half, e) for e in (1, 2, 4) for half in range(2)) + (
    (2, 0, 1), (1, 1, 2), (1, 0, 4), (2, 1, 4), (4, 1, 1), (4, 0, 2), (3, 0, 4), (5, 1, 2))


def kernel(q_hbm, k_hbm, v_hbm, cos_ref, sin_ref, out_ref,
           q_ref, k_ref, v_ref, in_sem, flat_kv, kv_ref, qs, qr, kvb, ost, k2, vT, key_place, s0, s1, s2, s3, p0, p1, p2, p3, mx, al, m_ref, acc_ref,
           q_send, q_recv, k1_send, k1_recv, k2_send, k2_recv, f_send, f_recv, o_send, o_recv):
    S, W = (s0, s1, s2, s3), (p0, p1, p2, p3)
    H = CW // 128
    me = Spot.own()
    others = [(d, dc) for d in ORDER for dc in (1, 0) if (d, dc) != (0, 0)]

    def remote(src, dst, send, recv, spot):
        return pltpu.make_async_remote_copy(src_ref=src, dst_ref=dst, send_sem=send, recv_sem=recv, device_id=spot.device, device_id_type=MESH)

    inputs = [
        pltpu.make_async_copy(src, dst, in_sem.at[n])
        for n, (src, dst) in enumerate(((k_hbm, k_ref), (v_hbm, v_ref), (q_hbm, q_ref)))
    ]
    for copy in inputs:
        copy.start()
    barrier = pltpu.get_barrier_semaphore()
    for d, dc in others:
        pl.semaphore_signal(barrier, inc=1, device_id=me.member(d, dc).device, device_id_type=MESH)
    for d in (1, 2, 4):
        pl.semaphore_signal(barrier, inc=1, device_id=me.cousin(d).device, device_id_type=MESH)

    row = lax.broadcasted_iota(jnp.int32, (KB, 128), 0)
    for ylo in range(2):
        z_at = ((row >> 7) & 1) ^ (3 * ((row >> 6) & 1))
        key_place[ylo] = (z_at * 2 + ((row >> 8) ^ ylo)) * 64 + (row & 63)

    acc_ref[...] = jnp.zeros_like(acc_ref)
    al[...] = jnp.zeros_like(al)
    for w in W[2:]:
        w[...] = jnp.zeros_like(w)

    @pl.loop(0, 16)
    def _(b):
        for h in range(4):
            vT[b, h, 128:VR, :] = jnp.ones((VR - 128, 128), BF16)

    for copy in inputs:
        copy.wait()
    k = k_ref[...].astype(F32).reshape(512, 128)
    flat_kv[0] = k * cos_ref[...] + pltpu.roll(k, 64, 1) * sin_ref[...]
    flat_kv[1] = v_ref[...].astype(F32).reshape(512, 128)
    for role in range(2):
        for h in range(8):
            kv_ref[role, h] = flat_kv[role, pl.ds(h, 64, stride=8), :].astype(BF16)

    def rotate_for(d):
        to = me.member(d, 0)
        x = q_ref[:, pl.ds(pl.multiple_of(to.chip * 16, 16), 16), :].astype(F32)
        for c in range(2):
            part = x[:, c * 8:(c + 1) * 8, :].reshape(512, 128)
            turned = part * cos_ref[...] + pltpu.roll(part, 64, 1) * sin_ref[...]
            flat = turned.astype(BF16).T
            for h in range(4):
                qs[to.chip * 2 + c, h] = flat[:, h * 128:(h + 1) * 128]

    for d in ORDER[:AHEAD]:
        rotate_for(d)
    pl.semaphore_wait(barrier, len(others) + 3)

    def kv_spot(role, src):
        return kvb.at[role, src.sx, src.part, pl.ds(pl.multiple_of(src.b[2] * 64, 64), 64), :]

    def first(d, dc):
        to = me.member(d, dc)
        return remote(kv_ref.at[to.core, to.chip], kv_spot(to.core, me), k1_send.at[d * 2 + dc], k1_recv.at[me.slot], to)

    for d, dc in others:
        first(d, dc).start()
    kvb[me.core, me.sx, me.part, pl.ds(pl.multiple_of(me.b[2] * 64, 64), 64), :] = kv_ref[me.core, me.chip]

    def queries_to(d, dc):
        to = me.member(d, dc)
        return remote(qs.at[to.head_block], qr.at[me.slot], q_send.at[d * 2 + dc], q_recv.at[me.slot], to)

    for n, d in enumerate(ORDER):
        if n >= AHEAD:
            rotate_for(d)
        for dc in (1, 0):
            if (d, dc) != (0, 0):
                queries_to(d, dc).start()
    qr[me.slot] = qs[me.head_block]

    for d, dc in others:
        frm = me.member(d, dc)
        remote(kv_ref.at[0, 0], kv_spot(me.core, frm), k1_send.at[d * 2 + dc], k1_recv.at[frm.slot], frm).wait_recv()

    def region(spot, half):
        return kvb.at[me.core, pl.ds(pl.multiple_of(place(spot.p[0], half) * 4, 4), 4), spot.part]

    def relay(a, half, e):
        r = region(me.cousin(a), half)
        n = (a ^ e) * 2 + half
        return remote(r, r, k2_send.at[n], k2_recv.at[n], me.cousin(e))

    def forward(d, half):
        r = region(me.cousin(d), half)
        return remote(r, r, f_send.at[d * 2 + half], f_recv.at[d * 2 + half], me.member(0, 1))

    def arrived(d, half):
        r = region(me.cousin(d), half)
        return remote(r, r, k2_send.at[d * 2 + half], k2_recv.at[d * 2 + half], me.cousin(d))

    def handed(d, half):
        r = kvb.at[1 - me.core, pl.ds(pl.multiple_of(place(me.cousin(d).p[0], half) * 4, 4), 4), me.cousin(d).part]
        return remote(r, r, f_send.at[d * 2 + half], f_recv.at[d * 2 + half], me.member(0, 1))

    def pass_on(d, half, *axes):
        arrived(d, half).wait_recv()
        for e in axes:
            relay(d, half, e).start()
        forward(d, half).start()

    def ready(d):
        for half in range(2):
            handed(d, half).wait_recv()
        spot = me.cousin(d)
        h = spot.part

        rows = pl.ds(pl.multiple_of(h * 128, 128), 128)
        for n in range(8):
            b = place(spot.p[0], n // 4) * 4 + n % 4
            vT[b, h, 0:128, :] = kvb[1, b, h].T
            wide = kvb[0, b, h].astype(F32) * SCALE
            hi = wide.astype(BF16)
            k2[b, 0, rows, :] = hi
            k2[b, 1, rows, :] = (wide - hi.astype(F32)).astype(BF16)

    for e, half in ((1, 1), (2, 0), (4, 1), (1, 0), (2, 1), (4, 0)):
        relay(0, half, e).start()
    for half in range(2):
        forward(0, half).start()

    ready(0)
    pass_on(2, 0, 1)
    pass_on(1, 1, 2)
    pass_on(1, 0, 4)
    pass_on(2, 1, 4)
    pass_on(4, 1, 1)
    pass_on(4, 0, 2)
    ready(1)
    ready(2)
    pass_on(3, 0, 4)
    pass_on(3, 1)
    ready(3)

    px = me.p[0]


    own_block = me.pair_block

    def early_block(k):
        g = k >> 1
        return own_block ^ ((1 - (g & 1)) * 4 + (1 - (g >> 1)) * 2 + (k & 1))

    def source(i, bz):
        return Spot(me.p, (i >> 2, (i >> 1) & 1, bz), i & 1)

    def rank(i):
        return (i & 4) + ((me.p[1] ^ ((i >> 1) & 1)) * 2) + (i & 1)

    def run(n):
        k = jnp.where(n < HEAD_RUNS, n, jnp.where(n < 2 * HEAD_RUNS, n - HEAD_RUNS, n >> 1))
        side = jnp.where(n < HEAD_RUNS, 0, jnp.where(n < 2 * HEAD_RUNS, 1, n & 1))
        return early_block(k), side

    def length(n):
        i, side = run(n)
        return jnp.where(side == 0, rank(i) + 1, jnp.where(px == 0, (i & 4) * 2, 4))

    def unit(at):
        n, r, seen = at
        i, side = run(n)
        mine = (px ^ (3 * (r >> 2))) * 4 + (r & 3)
        other = r + 4 * (1 - px)
        end = jnp.where(r + 1 == length(n), 1, 0)
        far = jnp.where(side == 1, 1, 0)
        done = end * jnp.where(far + (1 - (px | (i >> 2))) > 0, 1, 0)
        first_of = jnp.where(r == 0, 1, 0) * (1 - far)
        code = i + 8 * jnp.where(side == 0, mine, other) + 128 * first_of + 256 * done + 512 * end * (1 - far) + 1024 * far * (1 - seen)
        n1 = n + 1
        n1 = jnp.where(length(n1) == 0, n1 + 1, n1)
        n1 = jnp.where(length(n1) == 0, n1 + 1, n1)
        after = jnp.where(end == 1, jnp.minimum(n1, 15), n), jnp.where(end == 1, 0, r + 1), seen | far
        return code, after

    def qblock(u):
        return u & 7

    def kblock(u):
        return (u >> 3) & 15

    def queries_in(u):
        @pl.loop(0, (u >> 7) & 1)
        def _(_):
            i = qblock(u)
            for bz in range(2):
                s = 2 * i + bz

                @pl.when(s != me.slot)
                def _():
                    remote(qs.at[0], qr.at[s], q_send.at[0], q_recv.at[s], me.member(1, 0)).wait_recv()

    def qk_stage(u, slot, pieces=range(QW // CW)):
        i, b = qblock(u), kblock(u)
        for n in pieces:
            cols = pl.ds(n * CW, CW)
            kk = jnp.concatenate([k2[b, 0], k2[b, 1]], axis=1)
            qq = jnp.concatenate([qr[2 * i + (n * H + h) // 4, (n * H + h) % 4] for h in range(H)], axis=1)
            qq = jnp.concatenate([qq, qq], axis=0)
            s = jnp.dot(kk, qq, preferred_element_type=F32)
            S[slot][:, cols] = s
            mx[slot, :, cols] = jnp.max(s, axis=0, keepdims=True)

    def mask(u, slot):
        @pl.loop(0, (u >> 9) & 1)
        def _(_):
            here = source(qblock(u), 0)
            key_at = key_place[me.p[1] ^ here.b[1]]
            lane = lax.broadcasted_iota(jnp.int32, (1, 128), 1) >> 3
            for n in range(QW // 128):
                cols = pl.ds(n * 128, 128)
                query_at = lane + (source(qblock(u), n // 4).sy * 64 + n % 4 * 16)
                s = jnp.where(key_at <= query_at, S[slot][:, cols], NEG)
                S[slot][:, cols] = s
                mx[slot, :, cols] = jnp.max(s, axis=0, keepdims=True)

    def soft_stage(u, slot, pieces=range(QW // CW)):
        i = qblock(u)
        for n in pieces:
            cols = pl.ds(n * CW, CW)
            m_old = jnp.where((u >> 7) & 1 == 1, NEG, m_ref[i, :, cols])
            m_new = jnp.maximum(m_old, mx[slot, :, cols])
            m_ref[i, :, cols] = m_new
            al[slot, :, cols] = jnp.exp2(m_old - m_new)
            w = jnp.exp2(S[slot][:, cols] - m_new).astype(BF16)
            for h in range(H):
                W[slot][n * H + h] = w[:, h * 128:(h + 1) * 128]

    def pv_stage(u, slot):
        i, b = qblock(u), kblock(u)
        for n in range(QW // CW):
            cols = pl.ds(n * CW, CW)
            ww = jnp.concatenate([W[slot][n * H + h] for h in range(H)], axis=1)
            vv = jnp.concatenate([vT[b, h] for h in range(4)], axis=1)
            acc_ref[i, :, cols] = acc_ref[i, :, cols] * al[slot, :, cols] + jnp.dot(vv, ww, preferred_element_type=F32)

    def outputs_to(s):
        to = Spot(me.p, (s >> 3, (s >> 2) & 1, s & 1), (s >> 1) & 1)
        heads = pl.ds(pl.multiple_of(me.head_block * 8, 8), 8)
        return remote(ost.at[s], out_ref.at[:, heads, :], o_send.at[s], o_recv.at[me.head_block], to)

    def fin(u):
        @pl.loop(0, (u >> 8) & 1)
        def _(_):
            i = qblock(u)
            o = acc_ref[i, 0:128, :] * (1.0 / acc_ref[i, 128:129, :])
            for bz in range(2):
                for t in range(2):
                    c0 = bz * 512 + t * 256
                    ost[2 * i + bz, pl.ds(t * 32, 32)] = o[:, c0:c0 + 256].T.reshape(32, 8, 128).astype(BF16)
            for bz in range(2):
                s = 2 * i + bz

                @pl.when(s != me.slot)
                def _():
                    outputs_to(s).start()

                @pl.when(s == me.slot)
                def _():
                    out_ref[:, pl.ds(pl.multiple_of(me.head_block * 8, 8), 8), :] = ost[s]

    def other_keys(u):
        @pl.loop(0, (u >> 10) & 1)
        def _(_):
            pass_on(7, 0)
            pass_on(7, 1)
            for d in range(4, 8):
                ready(d)

    def any_of(bits, units):
        got = units[0] | units[1]
        return jnp.where((got & bits) != 0, 1, 0)

    def step(old, now, new, at, cur, nxt):
        if new is None:
            for n in range(2):
                soft_stage(now[n], cur + n)
            for n in range(2):
                pv_stage(old[n], nxt + n)
            for n in range(2):
                fin(old[n])
            return None

        @pl.loop(0, any_of(128 + 1024, new))
        def _(_):
            for n in range(2):
                queries_in(new[n])
                other_keys(new[n])

        ahead, at = take(at)
        for n in range(2):
            for piece in range(QW // CW):
                qk_stage(new[n], nxt + n, (piece,))
                soft_stage(now[n], cur + n, (piece,))
        for n in range(2):
            pv_stage(old[n], nxt + n)

        @pl.loop(0, jnp.maximum(any_of(512, new), any_of(256, old)))
        def _(_):
            for n in range(2):
                mask(new[n], nxt + n)
            for n in range(2):
                fin(old[n])

        return ahead, at

    def take(at):
        u, at = unit(at)
        v, at = unit(at)
        return (u, v), at

    z = jnp.int32(0)
    u01, at = take((z, z, z))
    for n in range(2):
        queries_in(u01[n])
        qk_stage(u01[n], n)
        mask(u01[n], n)
    new, at = take(at)

    dummy = (u01[0] & 127,) * 2

    def steps(t, carry):
        old, now, new, at = carry

        @pl.loop(0, jnp.where(t == 2, 1, 0))
        def _(_):
            pass_on(5, 1, 2)
            pass_on(5, 0)
            pass_on(6, 0)
            pass_on(6, 1)

        new2, at = step(old, now, new, at, 0, 2)
        new3, at = step(now, new, new2, at, 2, 0)
        return new, new2, new3, at

    old, now, new, at = lax.fori_loop(0, 16, steps, (dummy, u01, new, at))
    step(old, now, new, at, 0, 2)
    step(now, new, None, None, 2, 0)
    for n in range(2):
        pv_stage(new[n], 2 + n)
    for n in range(2):
        fin(new[n])

    for d, dc in others:
        first(d, dc).wait_send()
        queries_to(d, dc).wait_send()
        frm = me.member(d, dc)
        outputs_to(frm.slot).wait_send()
        heads = pl.ds(pl.multiple_of(frm.head_block * 8, 8), 8)
        remote(ost.at[0], out_ref.at[:, heads, :], o_send.at[frm.slot], o_recv.at[frm.head_block], frm).wait_recv()
    for d in range(8):
        for half in range(2):
            forward(d, half).wait_send()
    for relayed in RELAYS:
        relay(*relayed).wait_send()


def shards(queries, keys, values):
    rows, heads, width = queries.shape
    start = lax.axis_index(("sx", "sy")) * rows
    positions = start + jnp.arange(rows, dtype=jnp.int32)
    angles = positions.astype(F32)[:, None] * frequencies(width)[None, :]
    cosine, sine = jnp.cos(angles), jnp.sin(angles)
    cos2 = jnp.concatenate([cosine, cosine], axis=1)
    sin2 = jnp.concatenate([-sine, sine], axis=1)
    def eightfold(a):
        return jnp.broadcast_to(a[:, None, :], (rows, 8, width)).reshape(rows * 8, width)

    dma = pltpu.SemaphoreType.DMA
    return pl.pallas_call(
        kernel,
        out_shape=jax.ShapeDtypeStruct((rows, heads, width), BF16),
        in_specs=[pl.BlockSpec(memory_space=pltpu.HBM)] * 3 + [pl.BlockSpec(memory_space=pltpu.VMEM)] * 2,
        out_specs=pl.BlockSpec(memory_space=pltpu.VMEM),
        scratch_shapes=[
            pltpu.VMEM((rows, heads, width), BF16),
            pltpu.VMEM((rows, 8, width), BF16),
            pltpu.VMEM((rows, 8, width), BF16),
            dma((3,)),
            pltpu.VMEM((2, 512, 128), F32),
            pltpu.VMEM((2, 8, 64, 128), BF16),
            pltpu.VMEM((16, 4, 128, 128), BF16),
            pltpu.VMEM((16, 4, 128, 128), BF16),
            pltpu.VMEM((2, 16, 4, 128, 128), BF16),
            pltpu.VMEM((16, 64, 8, 128), BF16),
            pltpu.VMEM((16, 2, KB, 128), BF16),
            pltpu.VMEM((16, 4, VR, 128), BF16),
            pltpu.VMEM((2, KB, 128), jnp.int32),
            *[pltpu.VMEM((KB, QW), F32)] * 4,
            *[pltpu.VMEM((8, KB, 128), BF16)] * 4,
            pltpu.VMEM((4, 1, QW), F32),
            pltpu.VMEM((4, 1, QW), F32),
            pltpu.VMEM((8, 1, QW), F32),
            pltpu.VMEM((8, VR, QW), F32),
            *[dma((16,))] * 10,
        ],
        compiler_params=pltpu.CompilerParams(
            collective_id=0, has_side_effects=True, vmem_limit_bytes=40 << 20
        ),
        name="fused",
    )(
        *(pltpu.with_memory_space_constraint(a, pltpu.HBM) for a in (queries, keys, values)),
        eightfold(cos2),
        eightfold(sin2),
    )


def solution(mesh):
    placed = P(("sx", "sy"), None, None)
    return jax.shard_map(
        shards, mesh=mesh, in_specs=(placed, placed, placed), out_specs=placed, check_vma=False
    )
```
